32 devices in a mesh: ty: 16 (over z, y, core), tx: 2 (over x).
Axes of the slice: x: 2, y: 2, z: 4, core: 2. Of those that a mesh axis runs over, the one named last changes fastest.
Arguments:
- ctrl: float32 [16, 2, 512, 640], P('ty', 'tx'), may hold values from -6 to 6
- interp_wt: float32 [16, 2, 4, 128, 384], P('ty', 'tx'), may hold values from -0.3125 to 0.3125
- interp_cols: int32 [16, 2, 4, 384], P('ty', 'tx'), may hold values from 0 to 1023
- conv_wt: float32 [16, 2, 4, 128, 512], P('ty', 'tx'), may hold values from -0.25 to 0.25
- conv_cols: int32 [16, 2, 4, 512], P('ty', 'tx'), may hold values from 0 to 1023
- halo_index: int32 [16, 2, 8, 64], P('ty', 'tx'), may hold values from 0 to 511
- valid: int32 [16, 2], P('ty', 'tx'), may hold values from 256 to 512
Outputs:
- localized: float32 [16, 2, 512, 640], P('ty', 'tx')
The draws below stay inside these ranges and needn't reach their ends.
Inputs may be any that keep to these rules, and one draw needn't show every extreme that they name: `interp_cols`: indices into a tile's extended subgrid of 1024 rows; repeats are allowed. `conv_cols`: indices into a tile's extended subgrid; repeats are allowed. `halo_index`: owned row indices; repeats are allowed.
All inputs are finite; a program needn't handle non-finite values.
Results may differ from the reference program's by a relative error of at most 0.0001.
Values sent between devices are 32-bit elements; how exact they have to be, the bound alone decides.
A program may use at most 64 MiB of HBM per device.

```python
import jax
import jax.numpy as jnp
from jax import lax

NODES = 512
GRID = 512
HALO = 64
GROWS = 128
GCOLS = 384
CROWS = 128
CCOLS = 512
FEAT = 640
EXT = 1024
GBLK = 4
CBLK = 4
N_TY = 16
N_TX = 2


def with_ends(array, key, smallest, top_value):
    longest = array.shape.index(max(array.shape))
    spots = []
    for shift in (0, 1):
        where = [jax.random.randint(jax.random.fold_in(key, axis), (), 0, length) for axis, length in enumerate(array.shape)]
        where[longest] = (where[longest] + shift) % array.shape[longest]
        spots.append(tuple(where))
    return array.at[spots[0]].set(smallest).at[spots[1]].set(top_value)


def steps_of(stream_key, dims, cuts, low, largest):
    gain, own = 1.0, jax.random.fold_in(stream_key, 6)
    for position, blocks in cuts:
        steps = jnp.exp(jax.random.uniform(jax.random.fold_in(own, position), (blocks,), jnp.float32, low / len(cuts), largest / len(cuts)))
        gain = gain * jnp.repeat(steps, dims[position] // blocks).reshape([-1 if axis == position else 1 for axis in range(len(dims))])
    return gain


def scatter_about(rng, shape, scale, most, cuts=(), kind=jnp.bfloat16):
    gain = steps_of(rng, shape, cuts, -0.22, 0.18) if cuts else 1.0
    values = jax.random.normal(rng, shape, jnp.float32) * scale * gain
    return jnp.minimum(jnp.maximum(values, -most), most).astype(kind)


def setup_inputs(seed: int = 0) -> dict:
    keys = jax.random.split(jax.random.key(seed), 8)
    return {
        "ctrl": scatter_about(keys[0], (N_TY, N_TX, GRID, FEAT), 1.0, 6.0, ((0, 16), (1, 2)), jnp.float32),
        "interp_wt": scatter_about(keys[1], (N_TY, N_TX, GBLK, GROWS, GCOLS), GCOLS ** -0.5, 0.3125, ((0, 16), (1, 2)), jnp.float32),
        "interp_cols": with_ends(jax.random.randint(keys[2], (N_TY, N_TX, GBLK, GCOLS), 0, EXT), jax.random.fold_in(keys[2], 1), 0, EXT - 1).astype(jnp.int32),
        "conv_wt": scatter_about(keys[3], (N_TY, N_TX, CBLK, CROWS, CCOLS), CCOLS ** -0.5, 0.25, ((0, 16), (1, 2)), jnp.float32),
        "conv_cols": with_ends(jax.random.randint(keys[4], (N_TY, N_TX, CBLK, CCOLS), 0, EXT), jax.random.fold_in(keys[4], 1), 0, EXT - 1).astype(jnp.int32),
        "halo_index": with_ends(jax.random.randint(keys[5], (N_TY, N_TX, 8, HALO), 0, NODES), jax.random.fold_in(keys[5], 1), 0, NODES - 1).astype(jnp.int32),
        "valid": with_ends(jax.random.randint(keys[6], (N_TY, N_TX), GRID // 2, GRID + 1), jax.random.fold_in(keys[6], 1), GRID // 2, GRID).astype(jnp.int32),
    }


DIRECTIONS = ((-1, -1), (-1, 0), (-1, 1), (0, -1), (0, 1), (1, -1), (1, 0), (1, 1))


def neighbour(tiles, row_off, col_off):
    shifted = jnp.roll(tiles, -col_off, axis=1)
    edge = jnp.zeros_like(shifted[:1])
    if row_off == 1:
        return jnp.concatenate([shifted[1:], edge], axis=0)
    if row_off == -1:
        return jnp.concatenate([edge, shifted[:-1]], axis=0)
    return shifted


def over_tiles(func, *arrays):
    rows_t, cols_t = arrays[0].shape[:2]
    flat = tuple(item.reshape((rows_t * cols_t,) + item.shape[2:]) for item in arrays)
    result = lax.map(lambda packed: func(*packed), flat)
    return result.reshape((rows_t, cols_t) + result.shape[1:])


def forward_blocks(weights, cols, source):
    gathered = jnp.take(source, cols, axis=0)
    result = jnp.einsum("bgc,bcf->bgf", weights, gathered, precision=lax.Precision.HIGHEST)
    return result.reshape(-1, source.shape[1])


def adjoint_blocks(weights, cols, values):
    blocks = values.reshape(weights.shape[0], weights.shape[1], values.shape[1])
    contrib = jnp.einsum("bgc,bgf->bcf", weights, blocks, precision=lax.Precision.HIGHEST)
    return jax.ops.segment_sum(contrib.reshape(-1, values.shape[1]), cols.reshape(-1), num_segments=EXT)


def accumulate(contrib, halo_index):
    owned = contrib[:, :, :NODES]
    slots = contrib[:, :, NODES:].reshape(contrib.shape[0], contrib.shape[1], 8, HALO, FEAT)
    for slot_id in range(8):
        row_off, col_off = DIRECTIONS[slot_id]
        arrived = neighbour(slots[:, :, slot_id], row_off, col_off)
        owned = owned + over_tiles(lambda vals, idx: jax.ops.segment_sum(vals, idx, num_segments=NODES), arrived, halo_index[:, :, slot_id])
    return owned


def extend(owned, halo_index):
    sends = over_tiles(lambda field, idx: jnp.take(field, idx, axis=0), owned, halo_index)
    slots = []
    for slot_id in range(8):
        row_off, col_off = DIRECTIONS[slot_id]
        slots.append(neighbour(sends[:, :, slot_id], -row_off, -col_off))
    stacked = jnp.stack(slots, axis=2).reshape(owned.shape[0], owned.shape[1], 8 * HALO, FEAT)
    return jnp.concatenate([owned, stacked], axis=2)


def reference(ctrl, interp_wt, interp_cols, conv_wt, conv_cols, halo_index, valid):
    positions = jnp.arange(GRID, dtype=jnp.int32)
    mask = (positions[None, None, :] < valid[:, :, None]).astype(jnp.float32)[..., None]
    masked = ctrl * mask
    a_ext = over_tiles(adjoint_blocks, interp_wt, interp_cols, masked)
    summed = accumulate(a_ext, halo_index)
    b_ext = over_tiles(adjoint_blocks, conv_wt, conv_cols, summed)
    spread = accumulate(b_ext, halo_index)
    smooth = over_tiles(forward_blocks, conv_wt, conv_cols, extend(spread, halo_index))
    result = over_tiles(forward_blocks, interp_wt, interp_cols, extend(smooth, halo_index))
    return result * mask
```

```python
import functools

import jax
import jax.numpy as jnp
from jax import lax
from jax.experimental import pallas as pl
from jax.experimental.pallas import tpu as pltpu
from jax.sharding import PartitionSpec as P

MESH = pl.DeviceIdType.MESH
DIRECTIONS = ((-1, -1), (-1, 0), (-1, 1), (0, -1), (0, 1), (1, -1), (1, 0), (1, 1))
ORDER = (0, 2, 5, 7, 3, 4, 1, 6)
F32, BF16 = jnp.float32, jnp.bfloat16


def halves(x):
    hi = x.astype(BF16)
    return hi, (x - hi.astype(F32)).astype(BF16)


def dot(a, b):
    return jnp.dot(a, b, preferred_element_type=F32)


def dot_nt(a, b):
    return lax.dot_general(a, b, (((1,), (1,)), ((), ())), preferred_element_type=F32)


def kernel(
    n_ty, n_tx, chunks, valid_ref, ctrl_hbm, iwt_hbm, icols_ref, cwt_hbm, ccols_ref, halo_ref,
    out_ref, iwt_ref, cwt_ref, imat, imat_t, cmat, cmat_t, pick, pick_t, *rest,
):
    n_chunks = len(chunks)
    send_sem, recv_sem, load_sem, store_sem = rest[-4:]
    buffers = rest[:-4]
    own = buffers[:n_chunks]
    rhs = buffers[n_chunks : 2 * n_chunks]
    send = [buffers[(2 + e) * n_chunks : (3 + e) * n_chunks] for e in range(4)]
    recv = [buffers[(6 + e) * n_chunks : (7 + e) * n_chunks] for e in range(4)]
    loads = [pltpu.make_async_copy(iwt_hbm, iwt_ref, load_sem.at[0])]
    for c, (lo, width) in enumerate(chunks):
        loads.append(
            pltpu.make_async_copy(ctrl_hbm.at[:, lo : lo + width], own[c], load_sem.at[1 + c])
        )
    loads.append(pltpu.make_async_copy(cwt_hbm, cwt_ref, load_sem.at[1 + n_chunks]))
    for item in loads:
        item.start()
    ty, tx = lax.axis_index("ty"), lax.axis_index("tx")
    rows = out_ref.shape[0]
    n_own = own[0].shape[0]
    n_slot = recv[0][0].shape[0]
    slot = n_slot // 8
    extent = n_own + n_slot

    def there(off):
        return jnp.logical_and(ty + off >= 0, ty + off < n_ty)

    def peer(row_off, col_off):
        return ty + row_off, lax.rem(tx + col_off + n_tx, n_tx)

    barrier = pltpu.get_barrier_semaphore()
    for row_off, col_off in DIRECTIONS:
        @pl.when(there(row_off))
        def _():
            pl.semaphore_signal(
                barrier, inc=1, device_id=peer(row_off, col_off), device_id_type=MESH
            )

    def copy(e, c, d):
        sign = -1 if e < 2 else 1
        row_off, col_off = DIRECTIONS[d]
        piece = pl.ds(d * slot, slot)
        return pltpu.make_async_remote_copy(
            src_ref=send[e][c].at[piece],
            dst_ref=recv[e][c].at[piece],
            send_sem=send_sem.at[e, c, d],
            recv_sem=recv_sem.at[e, c, d],
            device_id=peer(sign * row_off, sign * col_off),
            device_id_type=MESH,
        )

    def each(e, c, sending, action):
        sign = -1 if e < 2 else 1
        for d in ORDER:
            row_off = DIRECTIONS[d][0] * (sign if sending else -sign)
            if row_off == 0:
                action(copy(e, c, d))
            else:
                pl.when(there(row_off))(functools.partial(lambda e, c, d: action(copy(e, c, d)), e, c, d))

    def start(e, c):
        each(e, c, True, lambda item: item.start())

    def arrived(e, c):
        each(e, c, False, lambda item: item.wait_recv())

    def spread(wt_ref, cols_ref, mat, mat_t, base=0, count=extent):
        blocks, height, width = wt_ref.shape
        for b in range(blocks):
            index = cols_ref[b : b + 1, :]
            place_of = lax.broadcasted_iota(jnp.int32, (count, width), 0) + base
            hot = (place_of == index).astype(F32).astype(BF16)
            hi, lo = halves(wt_ref[b])
            span = pl.ds(b * height, height)
            if mat is not None:
                mat[0, span], mat[1, span] = halves(dot_nt(hi, hot) + dot_nt(lo, hot))
            if mat_t is not None:
                part = pl.ds(base, count)
                mat_t[0, part, span], mat_t[1, part, span] = halves(dot_nt(hot, hi) + dot_nt(hot, lo))

    def product(mat, row0, count, col0, depth, c, base):
        a_hi = mat[0, row0 : row0 + count, col0 : col0 + depth]
        a_lo = mat[1, row0 : row0 + count, col0 : col0 + depth]
        b_hi, b_lo = rhs[c][0, base : base + depth], rhs[c][1, base : base + depth]
        return dot(a_hi, b_hi) + (dot(a_hi, b_lo) + dot(a_lo, b_hi))

    def gathered(e, c):
        hi, lo = halves(recv[e][c][...])
        return dot(pick_t[...], hi) + dot(pick_t[...], lo)

    def place(c, base, value):
        rhs[c][0, base : base + value.shape[0]], rhs[c][1, base : base + value.shape[0]] = halves(value)

    def picked(c):
        return dot(pick[...], rhs[c][0, :n_own]) + dot(pick[...], rhs[c][1, :n_own])

    for e in range(4):
        sign = -1 if e < 2 else 1
        for d, (row_off, _) in enumerate(DIRECTIONS):
            if row_off:
                @pl.when(jnp.logical_not(there(-sign * row_off)))
                def _():
                    for c in range(n_chunks):
                        piece = recv[e][c].at[pl.ds(d * slot, slot)]
                        piece[...] = jnp.zeros(piece.shape, F32)

    loads[0].wait()
    spread(iwt_ref, icols_ref, None, imat_t, n_own, n_slot)
    limit = valid_ref[0, 0]
    edge = jnp.int32(2)
    edge += jnp.where(there(-1), 3, 0) + jnp.where(there(1), 3, 0)
    pl.semaphore_wait(barrier, edge)

    def keep(width):
        return lax.broadcasted_iota(jnp.int32, (rows, width), 0) < limit

    for c, (lo, width) in enumerate(chunks):
        loads[1 + c].wait()
        place(c, 0, jnp.where(keep(width), own[c][...], 0.0))
        send[0][c][...] = product(imat_t, n_own, n_slot, 0, rows, c, 0)
        start(0, c)
    spread(iwt_ref, icols_ref, None, imat_t, 0, n_own)
    for c in range(n_chunks):
        own[c][...] = product(imat_t, 0, n_own, 0, rows, c, 0)
    halo = jnp.concatenate([halo_ref[d : d + 1, :] for d in range(8)], axis=1)
    hot = (lax.broadcasted_iota(jnp.int32, (n_own, n_slot), 0) == halo).astype(F32)
    loads[-1].wait()
    pick_t[...] = hot.astype(BF16)
    pick[...] = hot.T.astype(BF16)
    spread(cwt_ref, ccols_ref, None, cmat_t)
    for c in range(n_chunks):
        arrived(0, c)
        place(c, 0, own[c][...] + gathered(0, c))
        send[1][c][...] = product(cmat_t, n_own, n_slot, 0, n_own, c, 0)
        start(1, c)
        own[c][...] = product(cmat_t, 0, n_own, 0, n_own, c, 0)
    spread(cwt_ref, ccols_ref, cmat, None)
    spread(iwt_ref, icols_ref, imat, None)
    for c in range(n_chunks):
        arrived(1, c)
        place(c, 0, own[c][...] + gathered(1, c))
        send[2][c][...] = picked(c)
        start(2, c)
        own[c][...] = product(cmat, 0, n_own, 0, n_own, c, 0)
    for c in range(n_chunks):
        arrived(2, c)
        place(c, n_own, recv[2][c][...])
        place(c, 0, own[c][...] + product(cmat, 0, n_own, n_own, n_slot, c, n_own))
        send[3][c][...] = picked(c)
        start(3, c)
        own[c][...] = product(imat, 0, rows, 0, n_own, c, 0)
    stores = []
    for c, (lo, width) in enumerate(chunks):
        arrived(3, c)
        place(c, n_own, recv[3][c][...])
        total = own[c][...] + product(imat, 0, rows, n_own, n_slot, c, n_own)
        own[c][...] = jnp.where(keep(width), total, 0.0)
        stores.append(
            pltpu.make_async_copy(own[c], out_ref.at[:, lo : lo + width], store_sem.at[c])
        )
        stores[c].start()
    for e in range(4):
        for c in range(n_chunks):
            each(e, c, True, lambda item: item.wait_send())
    for item in stores:
        item.wait()

OWN_ORDER = (0, 2, 3, 4, 5, 7, 1, 6)
FAR_ORDER = (0, 2, 3, 4, 5, 7, 6, 1)


def stacked(x):
    hi, lo = halves(x)
    return hi, jnp.concatenate([hi, lo], axis=0)


def folded(x):
    half = x.shape[0] // 2
    return x[:half] + x[half:]


def pair_kernel(
    n_ty, cuts, valid_ref, ctrl_hbm, iwt_hbm, icols_ref, cwt_hbm, ccols_ref, halo_ref,
    out_ref, ctrl, iwt, cwt, cwt_f, ccols_f, halo_f, xt, imat, cmat, pick,
    zp, aslot, r1a, zf, r1o, r1f, bown, s2, r2, loc2, s3, r3, loc3, vacc,
    s4o, s4f, loc4, v_r, r4x, r4y, s5, r5, out_t, send_sem, recv_sem, load_sem,
):
    rows, feat = ctrl.shape
    half = feat // 2
    n_own, n_slot = pick.shape[1:]
    slot, group = n_slot // 8, n_slot // 4
    extent = n_own + n_slot
    n_x = 3 * group
    blocks = cwt.shape[0]
    ty, tx = lax.axis_index("ty"), lax.axis_index("tx")
    far = 1 - tx

    loads = [
        pltpu.make_async_copy(cwt_hbm, cwt, load_sem.at[0]),
        pltpu.make_async_copy(iwt_hbm, iwt, load_sem.at[1]),
        pltpu.make_async_copy(ctrl_hbm, ctrl, load_sem.at[2]),
    ]
    for item in loads:
        item.start()

    def there(off):
        return jnp.logical_and(ty + off >= 0, ty + off < n_ty)

    barrier = pltpu.get_barrier_semaphore()
    partners = [(0, 1), (-1, 0), (1, 0), (-1, 1), (1, 1)]
    for row_off, flip in partners:
        def greet(row_off=row_off, flip=flip):
            pl.semaphore_signal(
                barrier, inc=1, device_id=(ty + row_off, far if flip else tx), device_id_type=MESH
            )
        if row_off:
            pl.when(there(row_off))(greet)
        else:
            greet()

    flows = []

    class Flow:
        def __init__(self, src, dst, row_off, flip):
            self.row_off = row_off
            self.key = len(flows)
            flows.append(self)
            self.copy = pltpu.make_async_remote_copy(
                src_ref=src, dst_ref=dst, send_sem=send_sem.at[self.key], recv_sem=recv_sem.at[self.key],
                device_id=(ty + row_off, far if flip else tx), device_id_type=MESH,
            )

        def act(self, sign, action):
            if self.row_off:
                pl.when(there(sign * self.row_off))(action)
            else:
                action()

        def start(self):
            self.act(1, lambda: self.copy.start())

        def arrived(self):
            self.act(-1, lambda: self.copy.wait_recv())

        def sent(self):
            self.act(1, lambda: self.copy.wait_send())

    def go(*items):
        for item in items:
            item.start()
        return list(items)

    def wait(items):
        for item in items:
            item.arrived()

    def lane(count, width=group):
        return lax.broadcasted_iota(jnp.int32, (count, width), 1)

    def blend(first, second):
        return jnp.where(lane(first.shape[0]) < slot, first, second)

    def dense(mat, b, weights, index, order):
        where = index
        for place, d in enumerate(order):
            low = n_own + d * slot
            inside = jnp.logical_and(index >= low, index < low + slot)
            where = jnp.where(inside, index + (place - d) * slot, where)
        height, width = weights.shape
        hot = lax.broadcasted_iota(jnp.int32, (extent, width), 0) == where
        _, both = stacked(weights)
        span = pl.ds(b * height, height)
        mat[0, span], mat[1, span] = halves(folded(dot_nt(both, hot.astype(F32).astype(BF16))))

    def choose(t, ref, order):
        halo = jnp.concatenate([ref[d : d + 1, :] for d in order], axis=1)
        hot = lax.broadcasted_iota(jnp.int32, (n_own, n_slot), 0) == halo
        pick[t] = hot.astype(F32).astype(BF16)

    def scatter(t, pieces, lo=0):
        _, both = stacked(jnp.concatenate(pieces, axis=1) if len(pieces) > 1 else pieces[0])
        return folded(dot_nt(both, pick[t, :, lo : lo + group * len(pieces)]))

    def apply(x, mat, lo, count):
        hi, both = x
        return folded(dot(both, mat[0, :, lo : lo + count])) + dot(hi, mat[1, :, lo : lo + count])

    def apply_nt(x, mat, lo, count):
        hi, both = x
        return folded(dot_nt(both, mat[0, :, lo : lo + count])) + dot_nt(hi, mat[1, :, lo : lo + count])

    def gather(t, both, lo, count):
        return folded(dot(both, pick[t, :, lo : lo + count]))

    def mine(lo, count):
        return pl.ds(pl.multiple_of(tx * half + lo, 16), count)

    def theirs(lo, count):
        return pl.ds(pl.multiple_of(far * half + lo, 16), count)

    def blank(ref):
        ref[...] = jnp.zeros(ref.shape, ref.dtype)

    @pl.when(jnp.logical_not(there(-1)))
    def _():
        for ref in (
            r1a.at[0], r1o.at[0], r1f.at[0], r2.at[0], r2.at[1], r2.at[2],
            r3.at[3], r3.at[4], r3.at[5], r4x.at[2], r4y.at[1], r5.at[1],
        ):
            blank(ref)

    @pl.when(jnp.logical_not(there(1)))
    def _():
        for ref in (
            r1a.at[1], r1o.at[2], r1f.at[1], r2.at[3], r2.at[4], r2.at[5],
            r3.at[0], r3.at[1], r3.at[2], r4x.at[0], r4y.at[0], r5.at[0],
        ):
            blank(ref)

    loads[0].wait()
    pl.semaphore_wait(barrier, 1 + jnp.where(there(-1), 2, 0) + jnp.where(there(1), 2, 0))
    tables = go(Flow(ccols_ref, ccols_f, 0, 1), Flow(halo_ref, halo_f, 0, 1))
    weights = go(*[Flow(cwt.at[b], cwt_f.at[b], 0, 1) for b in range(blocks)])

    limit = valid_ref[0, 0]
    loads[1].wait()
    for b in range(iwt.shape[0]):
        dense(imat, b, iwt[b], icols_ref[b : b + 1, :], OWN_ORDER)
    loads[2].wait()
    tile = 128
    for lo in range(0, feat, tile):
        live = lax.broadcasted_iota(jnp.int32, (rows, tile), 0) < limit
        piece = jnp.where(live, ctrl[:, lo : lo + tile], 0.0).T
        xt[0, lo : lo + tile], xt[1, lo : lo + tile] = halves(piece)
    for lo in (0, half):
        hi = xt[0, lo : lo + half]
        both = jnp.concatenate([hi, xt[1, lo : lo + half]], axis=0)
        value = apply((hi, both), imat, n_own, n_slot)
        for g in range(4):
            aslot[g, lo : lo + half] = value[:, g * group : (g + 1) * group]
    first = go(Flow(aslot.at[3], r1a.at[0], 1, 0), Flow(aslot.at[3], r1a.at[1], -1, 0))
    for lo in (0, half):
        hi = xt[0, lo : lo + half]
        both = jnp.concatenate([hi, xt[1, lo : lo + half]], axis=0)
        zp[lo : lo + half] = apply((hi, both), imat, 0, n_own)
    choose(0, halo_ref, OWN_ORDER)
    wait(first)
    for lo in (0, half):
        span = slice(lo, lo + half)
        zp[span] = zp[span] + scatter(0, [blend(r1a[0, span], r1a[1, span])], n_x)
    crossed = []
    for lo, count in cuts:
        span = pl.ds(lo, count)
        away, here = theirs(lo, count), mine(lo, count)
        crossed.append(go(
            Flow(zp.at[away], zf.at[span], 0, 1),
            Flow(aslot.at[1, away], r1o.at[1, span], 0, 1),
            Flow(aslot.at[0, away], r1o.at[0, span], 1, 1),
            Flow(aslot.at[2, away], r1o.at[2, span], -1, 1),
            Flow(aslot.at[0, here], r1f.at[0, span], 1, 0),
            Flow(aslot.at[2, here], r1f.at[1, span], -1, 0),
        ))
    for b in range(blocks):
        dense(cmat.at[0], b, cwt[b], ccols_ref[b : b + 1, :], OWN_ORDER)
    wait(tables)
    choose(1, halo_f, FAR_ORDER)
    for b in range(blocks):
        wait(weights[b : b + 1])
        dense(cmat.at[1], b, cwt_f[b], ccols_f[b : b + 1, :], FAR_ORDER)

    second, third, fourth, fifth = {}, {}, {}, {}
    n = len(cuts)

    def adjoint(c):
        lo, count = cuts[c]
        span = pl.ds(lo, count)
        here = mine(lo, count)
        wait(crossed[c])
        z = [
            zp[here] + scatter(0, [r1o[g, span] for g in range(3)]),
            zf[span] + scatter(1, [r1f[0, span], aslot[1, here], r1f[1, span]]),
        ]
        z = [stacked(item) for item in z]
        last = []
        for t in range(2):
            value = apply(z[t], cmat.at[t], n_own, n_slot)
            s2[t, span] = value[:, :group]
            loc2[t, span] = value[:, group : 2 * group]
            s2[3 + t, span] = value[:, 2 * group : n_x]
            last.append(value[:, n_x:])
        s2[2, span] = blend(last[0], last[1])
        s2[5, span] = blend(last[1], last[0])
        second[c] = go(*[Flow(s2.at[k, span], r2.at[k, span], 1 if k < 3 else -1, 0) for k in range(6)])
        for t in range(2):
            bown[t, span] = apply(z[t], cmat.at[t], 0, n_own)

    def middle(c):
        lo, count = cuts[c]
        span = pl.ds(lo, count)
        wait(second[c])
        slots = [
            [r2[1, span], loc2[1, span], r2[4, span], blend(r2[2, span], r2[5, span])],
            [r2[0, span], loc2[0, span], r2[3, span], blend(r2[5, span], r2[2, span])],
        ]
        last, w = [], []
        for t in range(2):
            w.append(stacked(bown[t, span] + scatter(t, slots[t])))
            value = gather(t, w[t][1], 0, n_slot)
            s3[t, span] = value[:, :group]
            loc3[t, span] = value[:, group : 2 * group]
            s3[3 + t, span] = value[:, 2 * group : n_x]
            last.append(value[:, n_x:])
        s3[2, span] = blend(last[0], last[1])
        s3[5, span] = blend(last[1], last[0])
        third[c] = go(*[Flow(s3.at[k, span], r3.at[k, span], -1 if k < 3 else 1, 0) for k in range(6)])
        for t in range(2):
            vacc[t, span] = apply_nt(w[t], cmat.at[t], 0, n_own)

    def forward(c):
        lo, count = cuts[c]
        span = pl.ds(lo, count)
        wait(third[c])
        slots = [
            [r3[1, span], loc3[1, span], r3[4, span], blend(r3[2, span], r3[5, span])],
            [r3[0, span], loc3[0, span], r3[3, span], blend(r3[5, span], r3[2, span])],
        ]
        v = [None, None]
        for t in (1, 0):
            extra = stacked(jnp.concatenate(slots[t], axis=1))
            v[t] = vacc[t, span] + apply_nt(extra, cmat.at[t], n_own, n_slot)
            vacc[t, span] = v[t]
        far_v = go(Flow(vacc.at[1, span], v_r.at[span], 0, 1))
        value = gather(0, stacked(v[0])[1], 0, n_slot)
        for g in range(3):
            s4o[g, span] = value[:, g * group : (g + 1) * group]
        s5[0, span] = value[:, n_x:]
        far_s = go(*[Flow(s4o.at[g, span], r4x.at[g, span], g - 1, 1) for g in range(3)])
        value = gather(1, stacked(v[1])[1], 0, n_x)
        s4f[0, span], s4f[1, span] = value[:, :group], value[:, 2 * group :]
        loc4[span] = value[:, group : 2 * group]
        near = go(
            Flow(s4f.at[0, span], r4y.at[0, span], -1, 0),
            Flow(s4f.at[1, span], r4y.at[1, span], 1, 0),
            Flow(s5.at[0, span], r5.at[0, 0, span], -1, 0),
            Flow(s5.at[0, span], r5.at[1, 0, span], 1, 0),
        )
        fourth[c] = far_v, far_s, near

    def relay(c):
        lo, count = cuts[c]
        span = pl.ds(lo, count)
        wait(fourth[c][0])
        s5[1, span] = gather(0, stacked(v_r[span])[1], n_x, group)
        fifth[c] = go(
            Flow(s5.at[1, span], r5.at[0, 1, span], -1, 0),
            Flow(s5.at[1, span], r5.at[1, 1, span], 1, 0),
        )

    def finish(q, c):
        lo, count = cuts[c]
        span = pl.ds(lo, count)
        if q:
            wait(fourth[c][1])
            wait(fifth[c])
            pieces = [v_r[span], r4x[0, span], r4x[1, span], r4x[2, span]]
        else:
            wait(fourth[c][2])
            pieces = [vacc[0, span], r4y[0, span], loc4[span], r4y[1, span]]
        pieces.append(blend(r5[0, q, span], r5[1, q, span]))
        both = stacked(jnp.concatenate(pieces, axis=1))
        out_t[theirs(lo, count) if q else mine(lo, count)] = apply_nt(both, imat, 0, extent)

    adjoint(0)
    for c in range(n):
        middle(c)
        if c + 1 < n:
            adjoint(c + 1)
        forward(c)
    for c in range(n):
        finish(0, c)
    for c in range(n):
        relay(c)
        finish(1, c)
    for lo in range(0, feat, tile):
        live = lax.broadcasted_iota(jnp.int32, (rows, tile), 0) < limit
        out_ref[:, lo : lo + tile] = jnp.where(live, out_t[lo : lo + tile].T, 0.0)
    for item in flows:
        item.sent()


def split(total, parts):
    unit = total // 16
    sizes = [16 * (unit // parts + (1 if k < unit % parts else 0)) for k in range(parts)]
    starts = [sum(sizes[:k]) for k in range(parts)]
    return tuple(zip(starts, sizes))


def pair_call(n_ty, ctrl, interp_wt, interp_cols, conv_wt, conv_cols, halo_index, valid):
    rows, feat = ctrl.shape[2:]
    n_own = conv_wt.shape[2] * conv_wt.shape[3]
    n_slot = halo_index.shape[2] * halo_index.shape[3]
    extent, group, half = n_own + n_slot, n_slot // 4, feat // 2
    cuts = split(half, 3)
    pin = functools.partial(pltpu.with_memory_space_constraint, memory_space=pltpu.HBM)
    hbm = pl.BlockSpec(memory_space=pltpu.HBM)
    vmem = pl.BlockSpec(memory_space=pltpu.VMEM)

    def f32(*shape):
        return pltpu.VMEM(shape, F32)

    def bf16(*shape):
        return pltpu.VMEM(shape, BF16)

    scratch = [
        f32(rows, feat), f32(*interp_wt.shape[2:]), f32(*conv_wt.shape[2:]), f32(*conv_wt.shape[2:]),
        pltpu.VMEM(conv_cols.shape[2:], jnp.int32), pltpu.VMEM(halo_index.shape[2:], jnp.int32),
        bf16(2, feat, rows), bf16(2, rows, extent), bf16(2, 2, n_own, extent), bf16(2, n_own, n_slot),
        f32(feat, n_own), f32(4, feat, group), f32(2, feat, group), f32(half, n_own),
        f32(3, half, group), f32(2, half, group), f32(2, half, n_own),
        f32(6, half, group), f32(6, half, group), f32(2, half, group),
        f32(6, half, group), f32(6, half, group), f32(2, half, group), f32(2, half, n_own),
        f32(3, half, group), f32(2, half, group), f32(half, group), f32(half, n_own),
        f32(3, half, group), f32(2, half, group), f32(2, half, group), f32(2, 2, half, group),
        f32(feat, rows),
    ]
    flows = 2 + conv_wt.shape[2] + 2 + 28 * len(cuts)
    scratch += [pltpu.SemaphoreType.DMA((flows,))] * 2 + [pltpu.SemaphoreType.DMA((3,))]
    return pl.pallas_call(
        functools.partial(pair_kernel, n_ty, cuts),
        out_shape=jax.ShapeDtypeStruct((rows, feat), F32),
        in_specs=[pl.BlockSpec(memory_space=pltpu.SMEM), hbm, hbm, vmem, hbm, vmem, vmem],
        out_specs=vmem,
        scratch_shapes=scratch,
        compiler_params=pltpu.CompilerParams(
            collective_id=0, has_side_effects=True, vmem_limit_bytes=52 * 1024 * 1024
        ),
    )(
        valid, pin(ctrl[0, 0]), pin(interp_wt[0, 0]), pin(interp_cols[0, 0]), pin(conv_wt[0, 0]),
        pin(conv_cols[0, 0]), pin(halo_index[0, 0]),
    )


def pairs_fit(n_tx, ctrl, halo_index):
    slot = halo_index.shape[3]
    return n_tx == 2 and halo_index.shape[2] == 8 and slot == 64 and ctrl.shape[3] % 128 == 0


def solution(mesh):
    n_ty, n_tx = mesh.shape["ty"], mesh.shape["tx"]

    def body(ctrl, interp_wt, interp_cols, conv_wt, conv_cols, halo_index, valid):
        rows, feat = ctrl.shape[2:]
        n_own = conv_wt.shape[2] * conv_wt.shape[3]
        n_slot = halo_index.shape[2] * halo_index.shape[3]
        extent = n_own + n_slot
        if pairs_fit(n_tx, ctrl, halo_index) and rows == n_own:
            args = ctrl, interp_wt, interp_cols, conv_wt, conv_cols, halo_index, valid
            return pair_call(n_ty, *args)[None, None]
        tiles = feat // 128
        first = 128 * max(tiles - tiles // 2, 1)
        chunks = ((0, first), (first, feat - first)) if feat > first else ((0, feat),)
        widths = [width for _, width in chunks]
        pin = functools.partial(pltpu.with_memory_space_constraint, memory_space=pltpu.HBM)
        hbm = pl.BlockSpec(memory_space=pltpu.HBM)
        vmem = pl.BlockSpec(memory_space=pltpu.VMEM)
        scratch = [
            pltpu.VMEM(interp_wt.shape[2:], F32),
            pltpu.VMEM(conv_wt.shape[2:], F32),
            pltpu.VMEM((2, rows, extent), BF16),
            pltpu.VMEM((2, extent, rows), BF16),
            pltpu.VMEM((2, n_own, extent), BF16),
            pltpu.VMEM((2, extent, n_own), BF16),
            pltpu.VMEM((n_slot, n_own), BF16),
            pltpu.VMEM((n_own, n_slot), BF16),
        ]
        assert rows == n_own
        scratch += [pltpu.VMEM((n_own, width), F32) for width in widths]
        scratch += [pltpu.VMEM((2, extent, width), BF16) for width in widths]
        scratch += [pltpu.VMEM((n_slot, width), F32) for _ in range(8) for width in widths]
        scratch += [pltpu.SemaphoreType.DMA((4, len(chunks), 8))] * 2
        scratch += [pltpu.SemaphoreType.DMA((2 + len(chunks),)), pltpu.SemaphoreType.DMA((len(chunks),))]
        out = pl.pallas_call(
            functools.partial(kernel, n_ty, n_tx, chunks),
            out_shape=jax.ShapeDtypeStruct((rows, feat), F32),
            in_specs=[pl.BlockSpec(memory_space=pltpu.SMEM), hbm, hbm, vmem, hbm, vmem, vmem],
            out_specs=pl.BlockSpec(memory_space=pl.ANY),
            scratch_shapes=scratch,
            compiler_params=pltpu.CompilerParams(
                collective_id=0, has_side_effects=True, vmem_limit_bytes=44 * 1024 * 1024
            ),
        )(
            valid, pin(ctrl[0, 0]), pin(interp_wt[0, 0]), pin(interp_cols[0, 0]), pin(conv_wt[0, 0]),
            pin(conv_cols[0, 0]), pin(halo_index[0, 0]),
        )
        return out[None, None]

    placed = (
        P("ty", "tx", None, None),
        P("ty", "tx", None, None, None),
        P("ty", "tx", None, None),
        P("ty", "tx", None, None, None),
        P("ty", "tx", None, None),
        P("ty", "tx", None, None),
        P("ty", "tx"),
    )
    return jax.shard_map(
        body, mesh=mesh, in_specs=placed, out_specs=P("ty", "tx", None, None), check_vma=False
    )
```

```python
import functools

import jax
import jax.numpy as jnp
from jax import lax
from jax.experimental import pallas as pl
from jax.experimental.pallas import tpu as pltpu
from jax.sharding import PartitionSpec as P

MESH = pl.DeviceIdType.MESH
DIRECTIONS = ((-1, -1), (-1, 0), (-1, 1), (0, -1), (0, 1), (1, -1), (1, 0), (1, 1))
ORDER = (0, 2, 5, 7, 3, 4, 1, 6)
F32, BF16 = jnp.float32, jnp.bfloat16


def halves(x):
    hi = x.astype(BF16)
    return hi, (x - hi.astype(F32)).astype(BF16)


def dot(a, b):
    return jnp.dot(a, b, preferred_element_type=F32)


def dot_nt(a, b):
    return lax.dot_general(a, b, (((1,), (1,)), ((), ())), preferred_element_type=F32)


def kernel(
    n_ty, n_tx, chunks, valid_ref, ctrl_hbm, iwt_hbm, icols_ref, cwt_hbm, ccols_ref, halo_ref,
    out_ref, iwt_ref, cwt_ref, imat, imat_t, cmat, cmat_t, pick, pick_t, *rest,
):
    n_chunks = len(chunks)
    send_sem, recv_sem, load_sem, store_sem = rest[-4:]
    buffers = rest[:-4]
    own = buffers[:n_chunks]
    rhs = buffers[n_chunks : 2 * n_chunks]
    send = [buffers[(2 + e) * n_chunks : (3 + e) * n_chunks] for e in range(4)]
    recv = [buffers[(6 + e) * n_chunks : (7 + e) * n_chunks] for e in range(4)]
    loads = [pltpu.make_async_copy(iwt_hbm, iwt_ref, load_sem.at[0])]
    for c, (lo, width) in enumerate(chunks):
        loads.append(
            pltpu.make_async_copy(ctrl_hbm.at[:, lo : lo + width], own[c], load_sem.at[1 + c])
        )
    loads.append(pltpu.make_async_copy(cwt_hbm, cwt_ref, load_sem.at[1 + n_chunks]))
    for item in loads:
        item.start()
    ty, tx = lax.axis_index("ty"), lax.axis_index("tx")
    rows = out_ref.shape[0]
    n_own = own[0].shape[0]
    n_slot = recv[0][0].shape[0]
    slot = n_slot // 8
    extent = n_own + n_slot

    def there(off):
        return jnp.logical_and(ty + off >= 0, ty + off < n_ty)

    def peer(row_off, col_off):
        return ty + row_off, lax.rem(tx + col_off + n_tx, n_tx)

    barrier = pltpu.get_barrier_semaphore()
    for row_off, col_off in DIRECTIONS:
        @pl.when(there(row_off))
        def _():
            pl.semaphore_signal(
                barrier, inc=1, device_id=peer(row_off, col_off), device_id_type=MESH
            )

    def copy(e, c, d):
        sign = -1 if e < 2 else 1
        row_off, col_off = DIRECTIONS[d]
        piece = pl.ds(d * slot, slot)
        return pltpu.make_async_remote_copy(
            src_ref=send[e][c].at[piece],
            dst_ref=recv[e][c].at[piece],
            send_sem=send_sem.at[e, c, d],
            recv_sem=recv_sem.at[e, c, d],
            device_id=peer(sign * row_off, sign * col_off),
            device_id_type=MESH,
        )

    def each(e, c, sending, action):
        sign = -1 if e < 2 else 1
        for d in ORDER:
            row_off = DIRECTIONS[d][0] * (sign if sending else -sign)
            if row_off == 0:
                action(copy(e, c, d))
            else:
                pl.when(there(row_off))(functools.partial(lambda e, c, d: action(copy(e, c, d)), e, c, d))

    def start(e, c):
        each(e, c, True, lambda item: item.start())

    def arrived(e, c):
        each(e, c, False, lambda item: item.wait_recv())

    def spread(wt_ref, cols_ref, mat, mat_t, base=0, count=extent):
        blocks, height, width = wt_ref.shape
        for b in range(blocks):
            index = cols_ref[b : b + 1, :]
            place_of = lax.broadcasted_iota(jnp.int32, (count, width), 0) + base
            hot = (place_of == index).astype(F32).astype(BF16)
            hi, lo = halves(wt_ref[b])
            span = pl.ds(b * height, height)
            if mat is not None:
                mat[0, span], mat[1, span] = halves(dot_nt(hi, hot) + dot_nt(lo, hot))
            if mat_t is not None:
                part = pl.ds(base, count)
                mat_t[0, part, span], mat_t[1, part, span] = halves(dot_nt(hot, hi) + dot_nt(hot, lo))

    def product(mat, row0, count, col0, depth, c, base):
        a_hi = mat[0, row0 : row0 + count, col0 : col0 + depth]
        a_lo = mat[1, row0 : row0 + count, col0 : col0 + depth]
        b_hi, b_lo = rhs[c][0, base : base + depth], rhs[c][1, base : base + depth]
        return dot(a_hi, b_hi) + (dot(a_hi, b_lo) + dot(a_lo, b_hi))

    def gathered(e, c):
        hi, lo = halves(recv[e][c][...])
        return dot(pick_t[...], hi) + dot(pick_t[...], lo)

    def place(c, base, value):
        rhs[c][0, base : base + value.shape[0]], rhs[c][1, base : base + value.shape[0]] = halves(value)

    def picked(c):
        return dot(pick[...], rhs[c][0, :n_own]) + dot(pick[...], rhs[c][1, :n_own])

    for e in range(4):
        sign = -1 if e < 2 else 1
        for d, (row_off, _) in enumerate(DIRECTIONS):
            if row_off:
                @pl.when(jnp.logical_not(there(-sign * row_off)))
                def _():
                    for c in range(n_chunks):
                        piece = recv[e][c].at[pl.ds(d * slot, slot)]
                        piece[...] = jnp.zeros(piece.shape, F32)

    loads[0].wait()
    spread(iwt_ref, icols_ref, None, imat_t, n_own, n_slot)
    limit = valid_ref[0, 0]
    edge = jnp.int32(2)
    edge += jnp.where(there(-1), 3, 0) + jnp.where(there(1), 3, 0)
    pl.semaphore_wait(barrier, edge)

    def keep(width):
        return lax.broadcasted_iota(jnp.int32, (rows, width), 0) < limit

    for c, (lo, width) in enumerate(chunks):
        loads[1 + c].wait()
        place(c, 0, jnp.where(keep(width), own[c][...], 0.0))
        send[0][c][...] = product(imat_t, n_own, n_slot, 0, rows, c, 0)
        start(0, c)
    spread(iwt_ref, icols_ref, None, imat_t, 0, n_own)
    for c in range(n_chunks):
        own[c][...] = product(imat_t, 0, n_own, 0, rows, c, 0)
    halo = jnp.concatenate([halo_ref[d : d + 1, :] for d in range(8)], axis=1)
    hot = (lax.broadcasted_iota(jnp.int32, (n_own, n_slot), 0) == halo).astype(F32)
    loads[-1].wait()
    pick_t[...] = hot.astype(BF16)
    pick[...] = hot.T.astype(BF16)
    spread(cwt_ref, ccols_ref, None, cmat_t)
    for c in range(n_chunks):
        arrived(0, c)
        place(c, 0, own[c][...] + gathered(0, c))
        send[1][c][...] = product(cmat_t, n_own, n_slot, 0, n_own, c, 0)
        start(1, c)
        own[c][...] = product(cmat_t, 0, n_own, 0, n_own, c, 0)
    spread(cwt_ref, ccols_ref, cmat, None)
    spread(iwt_ref, icols_ref, imat, None)
    for c in range(n_chunks):
        arrived(1, c)
        place(c, 0, own[c][...] + gathered(1, c))
        send[2][c][...] = picked(c)
        start(2, c)
        own[c][...] = product(cmat, 0, n_own, 0, n_own, c, 0)
    for c in range(n_chunks):
        arrived(2, c)
        place(c, n_own, recv[2][c][...])
        place(c, 0, own[c][...] + product(cmat, 0, n_own, n_own, n_slot, c, n_own))
        send[3][c][...] = picked(c)
        start(3, c)
        own[c][...] = product(imat, 0, rows, 0, n_own, c, 0)
    stores = []
    for c, (lo, width) in enumerate(chunks):
        arrived(3, c)
        place(c, n_own, recv[3][c][...])
        total = own[c][...] + product(imat, 0, rows, n_own, n_slot, c, n_own)
        own[c][...] = jnp.where(keep(width), total, 0.0)
        stores.append(
            pltpu.make_async_copy(own[c], out_ref.at[:, lo : lo + width], store_sem.at[c])
        )
        stores[c].start()
    for e in range(4):
        for c in range(n_chunks):
            each(e, c, True, lambda item: item.wait_send())
    for item in stores:
        item.wait()

OWN_ORDER = (0, 2, 3, 4, 5, 7, 1, 6)
FAR_ORDER = (0, 2, 3, 4, 5, 7, 6, 1)


def stacked(x):
    hi, lo = halves(x)
    return hi, jnp.concatenate([hi, lo], axis=0)


def folded(x):
    half = x.shape[0] // 2
    return x[:half] + x[half:]


def pair_kernel(
    n_ty, cuts, valid_ref, ctrl_hbm, iwt_hbm, icols_ref, cwt_hbm, ccols_ref, halo_ref,
    out_ref, ctrl, iwt, cwt, cwt_f, ccols_f, halo_f, xt, imat, cmat, pick,
    zp, aslot, s1, r1, near, zf, r1o, bown, s2, r2, loc2, s3, r3, loc3, vacc,
    s4o, s4f, loc4, r4o, v_r, r4x, r4y, s5, r5, out_t, send_sem, recv_sem, load_sem,
):
    rows, feat = ctrl.shape
    half = feat // 2
    n_own, n_slot = pick.shape[1:]
    slot, group = n_slot // 8, n_slot // 4
    extent = n_own + n_slot
    n_x = 3 * group
    blocks = cwt.shape[0]
    ty, tx = lax.axis_index("ty"), lax.axis_index("tx")
    far = 1 - tx

    loads = [
        pltpu.make_async_copy(cwt_hbm, cwt, load_sem.at[0]),
        pltpu.make_async_copy(iwt_hbm, iwt, load_sem.at[1]),
        pltpu.make_async_copy(ctrl_hbm, ctrl, load_sem.at[2]),
    ]
    for item in loads:
        item.start()

    def there(off):
        return jnp.logical_and(ty + off >= 0, ty + off < n_ty)

    barrier = pltpu.get_barrier_semaphore()
    partners = [(0, 1), (-1, 0), (1, 0)]
    for row_off, flip in partners:
        def greet(row_off=row_off, flip=flip):
            pl.semaphore_signal(
                barrier, inc=1, device_id=(ty + row_off, far if flip else tx), device_id_type=MESH
            )
        if row_off:
            pl.when(there(row_off))(greet)
        else:
            greet()

    flows = []

    class Flow:
        def __init__(self, src, dst, row_off, flip):
            self.row_off = row_off
            self.key = len(flows)
            flows.append(self)
            self.copy = pltpu.make_async_remote_copy(
                src_ref=src, dst_ref=dst, send_sem=send_sem.at[self.key], recv_sem=recv_sem.at[self.key],
                device_id=(ty + row_off, far if flip else tx), device_id_type=MESH,
            )

        def act(self, sign, action):
            if self.row_off:
                pl.when(there(sign * self.row_off))(action)
            else:
                action()

        def start(self):
            self.act(1, lambda: self.copy.start())

        def arrived(self):
            self.act(-1, lambda: self.copy.wait_recv())

        def sent(self):
            self.act(1, lambda: self.copy.wait_send())

    def go(*items):
        for item in items:
            item.start()
        return list(items)

    def wait(items):
        for item in items:
            item.arrived()

    def lane(count, width=group):
        return lax.broadcasted_iota(jnp.int32, (count, width), 1)

    def blend(first, second):
        return jnp.where(lane(first.shape[0]) < slot, first, second)

    def packed(x):
        top, low = x[: x.shape[0] // 2], x[x.shape[0] // 2 :]
        low = pltpu.roll(low, slot, 1)
        return blend(top, low), blend(low, top)

    def unpacked(first, second):
        low = pltpu.roll(blend(second, first), slot, 1)
        return jnp.concatenate([blend(first, second), low], axis=0)

    def dense(mat, b, weights, index, order):
        where = index
        for place, d in enumerate(order):
            low = n_own + d * slot
            inside = jnp.logical_and(index >= low, index < low + slot)
            where = jnp.where(inside, index + (place - d) * slot, where)
        height, width = weights.shape
        hot = lax.broadcasted_iota(jnp.int32, (extent, width), 0) == where
        _, both = stacked(weights)
        span = pl.ds(b * height, height)
        mat[0, span], mat[1, span] = halves(folded(dot_nt(both, hot.astype(F32).astype(BF16))))

    def choose(t, ref, order):
        halo = jnp.concatenate([ref[d : d + 1, :] for d in order], axis=1)
        hot = lax.broadcasted_iota(jnp.int32, (n_own, n_slot), 0) == halo
        pick[t] = hot.astype(F32).astype(BF16)

    def scatter(t, pieces, lo=0):
        _, both = stacked(jnp.concatenate(pieces, axis=1) if len(pieces) > 1 else pieces[0])
        return folded(dot_nt(both, pick[t, :, lo : lo + group * len(pieces)]))

    def apply(x, mat, lo, count):
        hi, both = x
        return folded(dot(both, mat[0, :, lo : lo + count])) + dot(hi, mat[1, :, lo : lo + count])

    def apply_nt(x, mat, lo, count):
        hi, both = x
        return folded(dot_nt(both, mat[0, :, lo : lo + count])) + dot_nt(hi, mat[1, :, lo : lo + count])

    def gather(t, both, lo, count):
        return folded(dot(both, pick[t, :, lo : lo + count]))

    def mine(lo, count):
        return pl.ds(pl.multiple_of(tx * half + lo, 16), count)

    def theirs(lo, count):
        return pl.ds(pl.multiple_of(far * half + lo, 16), count)

    def blank(ref):
        ref[...] = jnp.zeros(ref.shape, ref.dtype)

    @pl.when(jnp.logical_not(there(-1)))
    def _():
        for ref in (
            r1.at[0], near.at[0], r2.at[0], r2.at[1], r2.at[2],
            r3.at[3], r3.at[4], r3.at[5], r4o.at[1], r4y.at[1], r5.at[1],
        ):
            blank(ref)

    @pl.when(jnp.logical_not(there(1)))
    def _():
        for ref in (
            r1.at[1], near.at[1], r2.at[3], r2.at[4], r2.at[5],
            r3.at[0], r3.at[1], r3.at[2], r4o.at[0], r4y.at[0], r5.at[0],
        ):
            blank(ref)

    loads[0].wait()
    pl.semaphore_wait(barrier, 1 + jnp.where(there(-1), 1, 0) + jnp.where(there(1), 1, 0))
    tables = go(Flow(ccols_ref, ccols_f, 0, 1), Flow(halo_ref, halo_f, 0, 1))
    weights = go(*[Flow(cwt.at[b], cwt_f.at[b], 0, 1) for b in range(blocks)])

    limit = valid_ref[0, 0]
    loads[1].wait()
    for b in range(iwt.shape[0]):
        dense(imat, b, iwt[b], icols_ref[b : b + 1, :], OWN_ORDER)
    loads[2].wait()
    tile = 128
    for lo in range(0, feat, tile):
        live = lax.broadcasted_iota(jnp.int32, (rows, tile), 0) < limit
        piece = jnp.where(live, ctrl[:, lo : lo + tile], 0.0).T
        xt[0, lo : lo + tile], xt[1, lo : lo + tile] = halves(piece)
    for lo in (0, half):
        hi = xt[0, lo : lo + half]
        both = jnp.concatenate([hi, xt[1, lo : lo + half]], axis=0)
        value = apply((hi, both), imat, n_own, n_slot)
        for g in range(4):
            aslot[g, lo : lo + half] = value[:, g * group : (g + 1) * group]
    s1[0], s1[1] = packed(aslot[3])
    first = go(Flow(s1.at[0], r1.at[0], 1, 0), Flow(s1.at[1], r1.at[1], -1, 0))
    sides = go(Flow(aslot.at[0], near.at[0], 1, 0), Flow(aslot.at[2], near.at[1], -1, 0))
    for lo in (0, half):
        hi = xt[0, lo : lo + half]
        both = jnp.concatenate([hi, xt[1, lo : lo + half]], axis=0)
        zp[lo : lo + half] = apply((hi, both), imat, 0, n_own)
    choose(0, halo_ref, OWN_ORDER)
    wait(first)
    extra = unpacked(r1[0], r1[1])
    for lo in (0, half):
        span = slice(lo, lo + half)
        zp[span] = zp[span] + scatter(0, [extra[span]], n_x)
    wait(sides)
    crossed = []
    for lo, count in cuts:
        span = pl.ds(lo, count)
        away = theirs(lo, count)
        crossed.append(go(
            Flow(zp.at[away], zf.at[span], 0, 1),
            Flow(near.at[0, away], r1o.at[0, span], 0, 1),
            Flow(aslot.at[1, away], r1o.at[1, span], 0, 1),
            Flow(near.at[1, away], r1o.at[2, span], 0, 1),
        ))
    for b in range(blocks):
        dense(cmat.at[0], b, cwt[b], ccols_ref[b : b + 1, :], OWN_ORDER)
    wait(tables)
    choose(1, halo_f, FAR_ORDER)
    for b in range(blocks):
        wait(weights[b : b + 1])
        dense(cmat.at[1], b, cwt_f[b], ccols_f[b : b + 1, :], FAR_ORDER)

    second, third, fourth, fifth, sixth, sides, whole = {}, {}, {}, {}, {}, {}, {}
    n = len(cuts)

    def adjoint(c):
        lo, count = cuts[c]
        span = pl.ds(lo, count)
        here = mine(lo, count)
        wait(crossed[c])
        z = [
            zp[here] + scatter(0, [r1o[g, span] for g in range(3)]),
            zf[span] + scatter(1, [near[0, here], aslot[1, here], near[1, here]]),
        ]
        z = [stacked(item) for item in z]
        last = []
        for t in range(2):
            value = apply(z[t], cmat.at[t], n_own, n_slot)
            s2[t, span] = value[:, :group]
            loc2[t, span] = value[:, group : 2 * group]
            s2[3 + t, span] = value[:, 2 * group : n_x]
            last.append(value[:, n_x:])
        s2[2, span] = blend(last[0], last[1])
        s2[5, span] = blend(last[1], last[0])
        second[c] = go(*[Flow(s2.at[k, span], r2.at[k, span], 1 if k < 3 else -1, 0) for k in range(6)])
        for t in range(2):
            bown[t, span] = apply(z[t], cmat.at[t], 0, n_own)

    def middle(c):
        lo, count = cuts[c]
        span = pl.ds(lo, count)
        wait(second[c])
        slots = [
            [r2[1, span], loc2[1, span], r2[4, span], blend(r2[2, span], r2[5, span])],
            [r2[0, span], loc2[0, span], r2[3, span], blend(r2[5, span], r2[2, span])],
        ]
        last, w = [], []
        for t in range(2):
            w.append(stacked(bown[t, span] + scatter(t, slots[t])))
            value = gather(t, w[t][1], 0, n_slot)
            s3[t, span] = value[:, :group]
            loc3[t, span] = value[:, group : 2 * group]
            s3[3 + t, span] = value[:, 2 * group : n_x]
            last.append(value[:, n_x:])
        s3[2, span] = blend(last[0], last[1])
        s3[5, span] = blend(last[1], last[0])
        third[c] = go(*[Flow(s3.at[k, span], r3.at[k, span], -1 if k < 3 else 1, 0) for k in range(6)])
        for t in range(2):
            vacc[t, span] = apply_nt(w[t], cmat.at[t], 0, n_own)

    def forward(c):
        lo, count = cuts[c]
        span = pl.ds(lo, count)
        wait(third[c])
        slots = [
            [r3[1, span], loc3[1, span], r3[4, span], blend(r3[2, span], r3[5, span])],
            [r3[0, span], loc3[0, span], r3[3, span], blend(r3[5, span], r3[2, span])],
        ]
        v = [None, None]
        for t in (1, 0):
            extra = stacked(jnp.concatenate(slots[t], axis=1))
            v[t] = vacc[t, span] + apply_nt(extra, cmat.at[t], n_own, n_slot)
            vacc[t, span] = v[t]
        whole[c] = go(Flow(vacc.at[1, span], v_r.at[span], 0, 1))
        value = gather(0, stacked(v[0])[1], 0, n_slot)
        for g in range(3):
            s4o[g, span] = value[:, g * group : (g + 1) * group]
        sides[c] = go(
            Flow(s4o.at[0, span], r4o.at[0, span], -1, 0), Flow(s4o.at[2, span], r4o.at[1, span], 1, 0)
        )
        fifth[0, c] = corner(0, c, value[:, n_x:])
        value = gather(1, stacked(v[1])[1], 0, n_x)
        s4f[0, span], s4f[1, span] = value[:, :group], value[:, 2 * group :]
        loc4[span] = value[:, group : 2 * group]
        fourth[c] = [
            Flow(s4f.at[0, span], r4y.at[0, span], -1, 0), Flow(s4f.at[1, span], r4y.at[1, span], 1, 0)
        ]

    def corner(q, c, value):
        lo, count = cuts[c]
        span = pl.ds(lo // 2, count // 2)
        s5[0, q, span], s5[1, q, span] = packed(value)
        return [Flow(s5.at[0, q, span], r5.at[0, q, span], -1, 0), Flow(s5.at[1, q, span], r5.at[1, q, span], 1, 0)]

    def leave(c):
        lo, count = cuts[c]
        span = pl.ds(lo, count)
        wait(sides[c])
        sixth[c] = go(
            Flow(r4o.at[0, span], r4x.at[0, span], 0, 1),
            Flow(s4o.at[1, span], r4x.at[1, span], 0, 1),
            Flow(r4o.at[1, span], r4x.at[2, span], 0, 1),
        )

    def spare(c):
        go(*fourth[c])
        go(*fifth[0, c])

    def relay(c):
        lo, count = cuts[c]
        span = pl.ds(lo, count)
        wait(whole[c])
        fifth[1, c] = corner(1, c, gather(0, stacked(v_r[span])[1], n_x, group))
        go(*fifth[1, c])

    def finish(q, c):
        lo, count = cuts[c]
        span = pl.ds(lo, count)
        if q:
            wait(sixth[c])
            pieces = [v_r[span], r4x[0, span], r4x[1, span], r4x[2, span]]
        else:
            wait(fourth[c])
            pieces = [vacc[0, span], r4y[0, span], loc4[span], r4y[1, span]]
        wait(fifth[q, c])
        span = pl.ds(lo // 2, count // 2)
        pieces.append(unpacked(r5[0, q, span], r5[1, q, span]))
        both = stacked(jnp.concatenate(pieces, axis=1))
        out_t[theirs(lo, count) if q else mine(lo, count)] = apply_nt(both, imat, 0, extent)

    for step in range(n + 3):
        for stage, lag in ((leave, 3), (forward, 2), (middle, 1), (adjoint, 0)):
            if 0 <= step - lag < n:
                stage(step - lag)
    for c in range(n):
        spare(c)
    for c in range(n):
        relay(c)
        finish(0, c)
    for c in range(n):
        finish(1, c)
    for lo in range(0, feat, tile):
        live = lax.broadcasted_iota(jnp.int32, (rows, tile), 0) < limit
        out_ref[:, lo : lo + tile] = jnp.where(live, out_t[lo : lo + tile].T, 0.0)
    for item in flows:
        item.sent()


def split(total, parts):
    unit = total // 16
    sizes = [16 * (unit // parts + (1 if k < unit % parts else 0)) for k in range(parts)]
    starts = [sum(sizes[:k]) for k in range(parts)]
    return tuple(zip(starts, sizes))


def pair_call(n_ty, ctrl, interp_wt, interp_cols, conv_wt, conv_cols, halo_index, valid):
    rows, feat = ctrl.shape[2:]
    n_own = conv_wt.shape[2] * conv_wt.shape[3]
    n_slot = halo_index.shape[2] * halo_index.shape[3]
    extent, group, half = n_own + n_slot, n_slot // 4, feat // 2
    cuts = split(half, 4)
    pin = functools.partial(pltpu.with_memory_space_constraint, memory_space=pltpu.HBM)
    hbm = pl.BlockSpec(memory_space=pltpu.HBM)
    vmem = pl.BlockSpec(memory_space=pltpu.VMEM)

    def f32(*shape):
        return pltpu.VMEM(shape, F32)

    def bf16(*shape):
        return pltpu.VMEM(shape, BF16)

    scratch = [
        f32(rows, feat), f32(*interp_wt.shape[2:]), f32(*conv_wt.shape[2:]), f32(*conv_wt.shape[2:]),
        pltpu.VMEM(conv_cols.shape[2:], jnp.int32), pltpu.VMEM(halo_index.shape[2:], jnp.int32),
        bf16(2, feat, rows), bf16(2, rows, extent), bf16(2, 2, n_own, extent), bf16(2, n_own, n_slot),
        f32(feat, n_own), f32(4, feat, group), f32(2, half, group), f32(2, half, group), f32(2, feat, group),
        f32(half, n_own), f32(3, half, group), f32(2, half, n_own),
        f32(6, half, group), f32(6, half, group), f32(2, half, group),
        f32(6, half, group), f32(6, half, group), f32(2, half, group), f32(2, half, n_own),
        f32(3, half, group), f32(2, half, group), f32(half, group), f32(2, half, group), f32(half, n_own),
        f32(3, half, group), f32(2, half, group), f32(2, 2, half // 2, group), f32(2, 2, half // 2, group),
        f32(feat, rows),
    ]
    flows = 2 + conv_wt.shape[2] + 4 + 28 * len(cuts)
    scratch += [pltpu.SemaphoreType.DMA((flows,))] * 2 + [pltpu.SemaphoreType.DMA((3,))]
    return pl.pallas_call(
        functools.partial(pair_kernel, n_ty, cuts),
        out_shape=jax.ShapeDtypeStruct((rows, feat), F32),
        in_specs=[pl.BlockSpec(memory_space=pltpu.SMEM), hbm, hbm, vmem, hbm, vmem, vmem],
        out_specs=vmem,
        scratch_shapes=scratch,
        compiler_params=pltpu.CompilerParams(
            collective_id=0, has_side_effects=True, vmem_limit_bytes=52 * 1024 * 1024
        ),
    )(
        valid, pin(ctrl[0, 0]), pin(interp_wt[0, 0]), pin(interp_cols[0, 0]), pin(conv_wt[0, 0]),
        pin(conv_cols[0, 0]), pin(halo_index[0, 0]),
    )


def pairs_fit(n_tx, ctrl, halo_index):
    slot = halo_index.shape[3]
    return n_tx == 2 and halo_index.shape[2] == 8 and slot == 64 and ctrl.shape[3] % 128 == 0


def solution(mesh):
    n_ty, n_tx = mesh.shape["ty"], mesh.shape["tx"]

    def body(ctrl, interp_wt, interp_cols, conv_wt, conv_cols, halo_index, valid):
        rows, feat = ctrl.shape[2:]
        n_own = conv_wt.shape[2] * conv_wt.shape[3]
        n_slot = halo_index.shape[2] * halo_index.shape[3]
        extent = n_own + n_slot
        if pairs_fit(n_tx, ctrl, halo_index) and rows == n_own:
            args = ctrl, interp_wt, interp_cols, conv_wt, conv_cols, halo_index, valid
            return pair_call(n_ty, *args)[None, None]
        tiles = feat // 128
        first = 128 * max(tiles - tiles // 2, 1)
        chunks = ((0, first), (first, feat - first)) if feat > first else ((0, feat),)
        widths = [width for _, width in chunks]
        pin = functools.partial(pltpu.with_memory_space_constraint, memory_space=pltpu.HBM)
        hbm = pl.BlockSpec(memory_space=pltpu.HBM)
        vmem = pl.BlockSpec(memory_space=pltpu.VMEM)
        scratch = [
            pltpu.VMEM(interp_wt.shape[2:], F32),
            pltpu.VMEM(conv_wt.shape[2:], F32),
            pltpu.VMEM((2, rows, extent), BF16),
            pltpu.VMEM((2, extent, rows), BF16),
            pltpu.VMEM((2, n_own, extent), BF16),
            pltpu.VMEM((2, extent, n_own), BF16),
            pltpu.VMEM((n_slot, n_own), BF16),
            pltpu.VMEM((n_own, n_slot), BF16),
        ]
        assert rows == n_own
        scratch += [pltpu.VMEM((n_own, width), F32) for width in widths]
        scratch += [pltpu.VMEM((2, extent, width), BF16) for width in widths]
        scratch += [pltpu.VMEM((n_slot, width), F32) for _ in range(8) for width in widths]
        scratch += [pltpu.SemaphoreType.DMA((4, len(chunks), 8))] * 2
        scratch += [pltpu.SemaphoreType.DMA((2 + len(chunks),)), pltpu.SemaphoreType.DMA((len(chunks),))]
        out = pl.pallas_call(
            functools.partial(kernel, n_ty, n_tx, chunks),
            out_shape=jax.ShapeDtypeStruct((rows, feat), F32),
            in_specs=[pl.BlockSpec(memory_space=pltpu.SMEM), hbm, hbm, vmem, hbm, vmem, vmem],
            out_specs=pl.BlockSpec(memory_space=pl.ANY),
            scratch_shapes=scratch,
            compiler_params=pltpu.CompilerParams(
                collective_id=0, has_side_effects=True, vmem_limit_bytes=44 * 1024 * 1024
            ),
        )(
            valid, pin(ctrl[0, 0]), pin(interp_wt[0, 0]), pin(interp_cols[0, 0]), pin(conv_wt[0, 0]),
            pin(conv_cols[0, 0]), pin(halo_index[0, 0]),
        )
        return out[None, None]

    placed = (
        P("ty", "tx", None, None),
        P("ty", "tx", None, None, None),
        P("ty", "tx", None, None),
        P("ty", "tx", None, None, None),
        P("ty", "tx", None, None),
        P("ty", "tx", None, None),
        P("ty", "tx"),
    )
    return jax.shard_map(
        body, mesh=mesh, in_specs=placed, out_specs=P("ty", "tx", None, None), check_vma=False
    )
```

```python
import functools

import jax
import jax.numpy as jnp
from jax import lax
from jax.experimental import pallas as pl
from jax.experimental.pallas import tpu as pltpu
from jax.sharding import PartitionSpec as P

MESH = pl.DeviceIdType.MESH
DIRECTIONS = ((-1, -1), (-1, 0), (-1, 1), (0, -1), (0, 1), (1, -1), (1, 0), (1, 1))
ORDER = (0, 2, 5, 7, 3, 4, 1, 6)
F32, BF16 = jnp.float32, jnp.bfloat16


def halves(x):
    hi = x.astype(BF16)
    return hi, (x - hi.astype(F32)).astype(BF16)


def dot(a, b):
    return jnp.dot(a, b, preferred_element_type=F32)


def dot_nt(a, b):
    return lax.dot_general(a, b, (((1,), (1,)), ((), ())), preferred_element_type=F32)


def kernel(
    n_ty, n_tx, chunks, valid_ref, ctrl_hbm, iwt_hbm, icols_ref, cwt_hbm, ccols_ref, halo_ref,
    out_ref, iwt_ref, cwt_ref, imat, imat_t, cmat, cmat_t, pick, pick_t, *rest,
):
    n_chunks = len(chunks)
    send_sem, recv_sem, load_sem, store_sem = rest[-4:]
    buffers = rest[:-4]
    own = buffers[:n_chunks]
    rhs = buffers[n_chunks : 2 * n_chunks]
    send = [buffers[(2 + e) * n_chunks : (3 + e) * n_chunks] for e in range(4)]
    recv = [buffers[(6 + e) * n_chunks : (7 + e) * n_chunks] for e in range(4)]
    loads = [pltpu.make_async_copy(iwt_hbm, iwt_ref, load_sem.at[0])]
    for c, (lo, width) in enumerate(chunks):
        loads.append(
            pltpu.make_async_copy(ctrl_hbm.at[:, lo : lo + width], own[c], load_sem.at[1 + c])
        )
    loads.append(pltpu.make_async_copy(cwt_hbm, cwt_ref, load_sem.at[1 + n_chunks]))
    for item in loads:
        item.start()
    ty, tx = lax.axis_index("ty"), lax.axis_index("tx")
    rows = out_ref.shape[0]
    n_own = own[0].shape[0]
    n_slot = recv[0][0].shape[0]
    slot = n_slot // 8
    extent = n_own + n_slot

    def there(off):
        return jnp.logical_and(ty + off >= 0, ty + off < n_ty)

    def peer(row_off, col_off):
        return ty + row_off, lax.rem(tx + col_off + n_tx, n_tx)

    barrier = pltpu.get_barrier_semaphore()
    for row_off, col_off in DIRECTIONS:
        @pl.when(there(row_off))
        def _():
            pl.semaphore_signal(
                barrier, inc=1, device_id=peer(row_off, col_off), device_id_type=MESH
            )

    def copy(e, c, d):
        sign = -1 if e < 2 else 1
        row_off, col_off = DIRECTIONS[d]
        piece = pl.ds(d * slot, slot)
        return pltpu.make_async_remote_copy(
            src_ref=send[e][c].at[piece],
            dst_ref=recv[e][c].at[piece],
            send_sem=send_sem.at[e, c, d],
            recv_sem=recv_sem.at[e, c, d],
            device_id=peer(sign * row_off, sign * col_off),
            device_id_type=MESH,
        )

    def each(e, c, sending, action):
        sign = -1 if e < 2 else 1
        for d in ORDER:
            row_off = DIRECTIONS[d][0] * (sign if sending else -sign)
            if row_off == 0:
                action(copy(e, c, d))
            else:
                pl.when(there(row_off))(functools.partial(lambda e, c, d: action(copy(e, c, d)), e, c, d))

    def start(e, c):
        each(e, c, True, lambda item: item.start())

    def arrived(e, c):
        each(e, c, False, lambda item: item.wait_recv())

    def spread(wt_ref, cols_ref, mat, mat_t, base=0, count=extent):
        blocks, height, width = wt_ref.shape
        for b in range(blocks):
            index = cols_ref[b : b + 1, :]
            place_of = lax.broadcasted_iota(jnp.int32, (count, width), 0) + base
            hot = (place_of == index).astype(F32).astype(BF16)
            hi, lo = halves(wt_ref[b])
            span = pl.ds(b * height, height)
            if mat is not None:
                mat[0, span], mat[1, span] = halves(dot_nt(hi, hot) + dot_nt(lo, hot))
            if mat_t is not None:
                part = pl.ds(base, count)
                mat_t[0, part, span], mat_t[1, part, span] = halves(dot_nt(hot, hi) + dot_nt(hot, lo))

    def product(mat, row0, count, col0, depth, c, base):
        a_hi = mat[0, row0 : row0 + count, col0 : col0 + depth]
        a_lo = mat[1, row0 : row0 + count, col0 : col0 + depth]
        b_hi, b_lo = rhs[c][0, base : base + depth], rhs[c][1, base : base + depth]
        return dot(a_hi, b_hi) + (dot(a_hi, b_lo) + dot(a_lo, b_hi))

    def gathered(e, c):
        hi, lo = halves(recv[e][c][...])
        return dot(pick_t[...], hi) + dot(pick_t[...], lo)

    def place(c, base, value):
        rhs[c][0, base : base + value.shape[0]], rhs[c][1, base : base + value.shape[0]] = halves(value)

    def picked(c):
        return dot(pick[...], rhs[c][0, :n_own]) + dot(pick[...], rhs[c][1, :n_own])

    for e in range(4):
        sign = -1 if e < 2 else 1
        for d, (row_off, _) in enumerate(DIRECTIONS):
            if row_off:
                @pl.when(jnp.logical_not(there(-sign * row_off)))
                def _():
                    for c in range(n_chunks):
                        piece = recv[e][c].at[pl.ds(d * slot, slot)]
                        piece[...] = jnp.zeros(piece.shape, F32)

    loads[0].wait()
    spread(iwt_ref, icols_ref, None, imat_t, n_own, n_slot)
    limit = valid_ref[0, 0]
    edge = jnp.int32(2)
    edge += jnp.where(there(-1), 3, 0) + jnp.where(there(1), 3, 0)
    pl.semaphore_wait(barrier, edge)

    def keep(width):
        return lax.broadcasted_iota(jnp.int32, (rows, width), 0) < limit

    for c, (lo, width) in enumerate(chunks):
        loads[1 + c].wait()
        place(c, 0, jnp.where(keep(width), own[c][...], 0.0))
        send[0][c][...] = product(imat_t, n_own, n_slot, 0, rows, c, 0)
        start(0, c)
    spread(iwt_ref, icols_ref, None, imat_t, 0, n_own)
    for c in range(n_chunks):
        own[c][...] = product(imat_t, 0, n_own, 0, rows, c, 0)
    halo = jnp.concatenate([halo_ref[d : d + 1, :] for d in range(8)], axis=1)
    hot = (lax.broadcasted_iota(jnp.int32, (n_own, n_slot), 0) == halo).astype(F32)
    loads[-1].wait()
    pick_t[...] = hot.astype(BF16)
    pick[...] = hot.T.astype(BF16)
    spread(cwt_ref, ccols_ref, None, cmat_t)
    for c in range(n_chunks):
        arrived(0, c)
        place(c, 0, own[c][...] + gathered(0, c))
        send[1][c][...] = product(cmat_t, n_own, n_slot, 0, n_own, c, 0)
        start(1, c)
        own[c][...] = product(cmat_t, 0, n_own, 0, n_own, c, 0)
    spread(cwt_ref, ccols_ref, cmat, None)
    spread(iwt_ref, icols_ref, imat, None)
    for c in range(n_chunks):
        arrived(1, c)
        place(c, 0, own[c][...] + gathered(1, c))
        send[2][c][...] = picked(c)
        start(2, c)
        own[c][...] = product(cmat, 0, n_own, 0, n_own, c, 0)
    for c in range(n_chunks):
        arrived(2, c)
        place(c, n_own, recv[2][c][...])
        place(c, 0, own[c][...] + product(cmat, 0, n_own, n_own, n_slot, c, n_own))
        send[3][c][...] = picked(c)
        start(3, c)
        own[c][...] = product(imat, 0, rows, 0, n_own, c, 0)
    stores = []
    for c, (lo, width) in enumerate(chunks):
        arrived(3, c)
        place(c, n_own, recv[3][c][...])
        total = own[c][...] + product(imat, 0, rows, n_own, n_slot, c, n_own)
        own[c][...] = jnp.where(keep(width), total, 0.0)
        stores.append(
            pltpu.make_async_copy(own[c], out_ref.at[:, lo : lo + width], store_sem.at[c])
        )
        stores[c].start()
    for e in range(4):
        for c in range(n_chunks):
            each(e, c, True, lambda item: item.wait_send())
    for item in stores:
        item.wait()

OWN_ORDER = (0, 2, 3, 4, 5, 7, 1, 6)
FAR_ORDER = (0, 2, 3, 4, 5, 7, 6, 1)


def stacked(x):
    hi, lo = halves(x)
    return hi, jnp.concatenate([hi, lo], axis=0)


def folded(x):
    half = x.shape[0] // 2
    return x[:half] + x[half:]


def pair_kernel(
    n_ty, cuts, valid_ref, ctrl_hbm, iwt_hbm, icols_hbm, cwt_hbm, ccols_hbm, halo_hbm,
    out_ref, icols_ref, ccols_ref, halo_ref, ctrl, iwt, cwt, cwt_f, ccols_f, halo_f, xt, imat, cmat, pick,
    zp, s1, near, zf, r1o, bown, s2, r2, loc2, s3, r3, loc3, vacc,
    s4o, r4o, r4x, v_r, s6, r6, loc6, s5, r5, out_t, out_v, send_sem, recv_sem, load_sem, store_sem,
):
    rows, feat = ctrl.shape
    half = feat // 2
    n_own, n_slot = pick.shape[1:]
    slot, group = n_slot // 8, n_slot // 4
    extent = n_own + n_slot
    n_x = 3 * group
    blocks = cwt.shape[0]
    ty, tx = lax.axis_index("ty"), lax.axis_index("tx")
    far = 1 - tx

    loads = [
        pltpu.make_async_copy(cwt_hbm, cwt, load_sem.at[0]),
        pltpu.make_async_copy(iwt_hbm, iwt, load_sem.at[1]),
        pltpu.make_async_copy(ctrl_hbm, ctrl, load_sem.at[2]),
        pltpu.make_async_copy(icols_hbm, icols_ref, load_sem.at[3]),
        pltpu.make_async_copy(ccols_hbm, ccols_ref, load_sem.at[4]),
        pltpu.make_async_copy(halo_hbm, halo_ref, load_sem.at[5]),
    ]
    for item in loads:
        item.start()

    def there(off):
        return jnp.logical_and(ty + off >= 0, ty + off < n_ty)

    barrier = pltpu.get_barrier_semaphore()
    partners = [(0, 1), (-1, 0), (1, 0)]
    for row_off, flip in partners:
        def greet(row_off=row_off, flip=flip):
            pl.semaphore_signal(
                barrier, inc=1, device_id=(ty + row_off, far if flip else tx), device_id_type=MESH
            )
        if row_off:
            pl.when(there(row_off))(greet)
        else:
            greet()

    flows, tags = [], {}

    class Flow:
        def __init__(self, src, dst, row_off, flip, tag=None):
            self.row_off = row_off
            self.tag = tag or len(flows)
            key = tags.setdefault(self.tag, [len(tags), None])[0]
            self.copy = pltpu.make_async_remote_copy(
                src_ref=src, dst_ref=dst, send_sem=send_sem.at[key], recv_sem=recv_sem.at[len(flows)],
                device_id=(ty + row_off, far if flip else tx), device_id_type=MESH,
            )
            flows.append(self)

        def act(self, sign, action):
            if self.row_off:
                pl.when(there(sign * self.row_off))(action)
            else:
                action()

        def start(self):
            before = tags[self.tag][1]
            if before is not None:
                before.sent()
            tags[self.tag][1] = self
            self.act(1, lambda: self.copy.start())

        def arrived(self):
            self.act(-1, lambda: self.copy.wait_recv())

        def sent(self):
            self.act(1, lambda: self.copy.wait_send())

    def go(*items):
        for item in items:
            item.start()
        return list(items)

    def wait(items):
        for item in items:
            item.arrived()

    def lane(count, width=group):
        return lax.broadcasted_iota(jnp.int32, (count, width), 1)

    def blend(first, second):
        return jnp.where(lane(first.shape[0]) < slot, first, second)

    def packed(x):
        top, low = x[: x.shape[0] // 2], x[x.shape[0] // 2 :]
        low = pltpu.roll(low, slot, 1)
        return blend(top, low), blend(low, top)

    def unpacked(first, second):
        low = pltpu.roll(blend(second, first), slot, 1)
        return jnp.concatenate([blend(first, second), low], axis=0)

    def dense(mat, b, weights, index, order):
        where = index
        for place, d in enumerate(order):
            low = n_own + d * slot
            inside = jnp.logical_and(index >= low, index < low + slot)
            where = jnp.where(inside, index + (place - d) * slot, where)
        height, width = weights.shape
        hot = lax.broadcasted_iota(jnp.int32, (extent, width), 0) == where
        _, both = stacked(weights)
        span = pl.ds(b * height, height)
        mat[0, span], mat[1, span] = halves(folded(dot_nt(both, hot.astype(F32).astype(BF16))))

    def choose(t, ref, order):
        halo = jnp.concatenate([ref[d : d + 1, :] for d in order], axis=1)
        hot = lax.broadcasted_iota(jnp.int32, (n_own, n_slot), 0) == halo
        pick[t] = hot.astype(F32).astype(BF16)

    def scatter(t, pieces, lo=0):
        value = jnp.concatenate(pieces, axis=1) if len(pieces) > 1 else pieces[0]
        return folded(dot_nt(stacked(value)[1], pick[t, :, lo : lo + value.shape[1]]))

    def apply(x, mat, lo, count):
        hi, both = x
        return folded(dot(both, mat[0, :, lo : lo + count])) + dot(hi, mat[1, :, lo : lo + count])

    def apply_nt(x, mat, lo, count):
        hi, both = x
        return folded(dot_nt(both, mat[0, :, lo : lo + count])) + dot_nt(hi, mat[1, :, lo : lo + count])

    def gather(t, both, lo, count):
        return folded(dot(both, pick[t, :, lo : lo + count]))

    def within(side, lo, count):
        start = side * lo + (1 - side) * (half - lo - count)
        return pl.ds(pl.multiple_of(start, 16), count)

    def placed(side, lo, count):
        start = side * (half + lo) + (1 - side) * (half - lo - count)
        return pl.ds(pl.multiple_of(start, 16), count)

    def mine(lo, count):
        return placed(tx, lo, count)

    def theirs(lo, count):
        return placed(far, lo, count)

    def blank(ref):
        ref[...] = jnp.zeros(ref.shape, ref.dtype)

    @pl.when(jnp.logical_not(there(-1)))
    def _():
        for ref in (near.at[0], r2.at[0], r3.at[1], r4o.at[2], r6.at[1], r5.at[1]):
            blank(ref)

    @pl.when(jnp.logical_not(there(1)))
    def _():
        for ref in (near.at[2], r2.at[1], r3.at[0], r4o.at[0], r6.at[0], r5.at[0]):
            blank(ref)

    loads[0].wait()
    pl.semaphore_wait(barrier, 1 + jnp.where(there(-1), 1, 0) + jnp.where(there(1), 1, 0))
    for item in loads[3:]:
        item.wait()
    tables = go(Flow(ccols_ref, ccols_f, 0, 1), Flow(halo_ref, halo_f, 0, 1))
    weights = go(Flow(cwt, cwt_f, 0, 1))

    limit = valid_ref[0, 0]
    loads[1].wait()
    for b in range(iwt.shape[0]):
        dense(imat, b, iwt[b], icols_ref[b : b + 1, :], OWN_ORDER)
    loads[2].wait()
    tile = 128
    for lo in range(0, feat, tile):
        live = lax.broadcasted_iota(jnp.int32, (rows, tile), 0) < limit
        piece = jnp.where(live, ctrl[:, lo : lo + tile], 0.0).T
        xt[0, lo : lo + tile], xt[1, lo : lo + tile] = halves(piece)
    last = []
    for q in range(2):
        span = slice(q * half, (q + 1) * half)
        both = jnp.concatenate([xt[0, span], xt[1, span]], axis=0)
        value = apply((xt[0, span], both), imat, n_own, n_slot)
        s1[0, q], near[1, q], s1[1, q] = (value[:, g * group : (g + 1) * group] for g in range(3))
        last.append(value[:, n_x:])
    s1[0, 2], s1[1, 2] = packed(jnp.concatenate(last, axis=0))
    first = go(Flow(s1.at[0], near.at[0], 1, 0), Flow(s1.at[1], near.at[2], -1, 0))
    for q in range(2):
        span = slice(q * half, (q + 1) * half)
        both = jnp.concatenate([xt[0, span], xt[1, span]], axis=0)
        zp[span] = apply((xt[0, span], both), imat, 0, n_own)
    choose(0, halo_ref, OWN_ORDER)
    wait(first)
    extra = unpacked(near[0, 2], near[2, 2])
    for q in range(2):
        span = slice(q * half, (q + 1) * half)
        zp[span] = zp[span] + scatter(0, [extra[span]], n_x)
    crossed = []
    for lo, count in cuts:
        span = pl.ds(lo, count)
        crossed.append(go(
            Flow(zp.at[theirs(lo, count)], zf.at[span], 0, 1),
            Flow(near.at[:, far, within(far, lo, count)], r1o.at[:, span], 0, 1),
        ))
    for b in range(blocks):
        dense(cmat.at[0], b, cwt[b], ccols_ref[b : b + 1, :], OWN_ORDER)
    wait(tables)
    choose(1, halo_f, FAR_ORDER)
    wait(weights)
    for b in range(blocks):
        dense(cmat.at[1], b, cwt_f[b], ccols_f[b : b + 1, :], FAR_ORDER)

    second, third, fourth, fifth, sixth, sides, whole = {}, {}, {}, {}, {}, {}, {}
    n = len(cuts)

    def swap(c, sent, got, kept, sign, tag, value):
        span = pl.ds(*cuts[c])
        last = []
        for t in range(2):
            sent[0, t, span], kept[t, span] = value[t][:, :group], value[t][:, group : 2 * group]
            sent[1, t, span] = value[t][:, 2 * group : n_x]
            last.append(value[t][:, n_x:])
        sent[0, 2, span], sent[1, 2, span] = blend(last[0], last[1]), blend(last[1], last[0])
        return go(*[
            Flow(sent.at[k, :, span], got.at[k, :, span], sign - 2 * k * sign, 0, (tag, k)) for k in range(2)
        ])

    def swapped(c, got, kept):
        span = pl.ds(*cuts[c])
        return [
            jnp.concatenate([
                got[0, 1 - t, span], kept[1 - t, span], got[1, 1 - t, span],
                blend(got[t, 2, span], got[1 - t, 2, span]),
            ], axis=1)
            for t in range(2)
        ]

    def adjoint(c):
        lo, count = cuts[c]
        span = pl.ds(lo, count)
        here = within(tx, lo, count)
        wait(crossed[c])
        z = [
            zp[mine(lo, count)] + scatter(0, [r1o[g, span] for g in range(3)]),
            zf[span] + scatter(1, [near[g, tx, here] for g in range(3)]),
        ]
        z = [stacked(item) for item in z]
        second[c] = swap(c, s2, r2, loc2, 1, "b", [apply(z[t], cmat.at[t], n_own, n_slot) for t in range(2)])
        for t in range(2):
            bown[t, span] = apply(z[t], cmat.at[t], 0, n_own)

    def middle(c):
        span = pl.ds(*cuts[c])
        wait(second[c])
        slots = swapped(c, r2, loc2)
        w = [stacked(bown[t, span] + scatter(t, [slots[t]])) for t in range(2)]
        third[c] = swap(c, s3, r3, loc3, -1, "w", [gather(t, w[t][1], 0, n_slot) for t in range(2)])
        for t in range(2):
            vacc[t, span] = apply_nt(w[t], cmat.at[t], 0, n_own)

    def forward(c):
        lo, count = cuts[c]
        span, part = pl.ds(lo, count), pl.ds(lo // 2, count // 2)
        wait(third[c])
        slots = swapped(c, r3, loc3)
        v = [None, None]
        for t in (1, 0):
            v[t] = vacc[t, span] + apply_nt(stacked(slots[t]), cmat.at[t], n_own, n_slot)
            vacc[t, span] = v[t]
            if t:
                whole[c] = go(Flow(vacc.at[1, span], v_r.at[span], 0, 1))
        value = gather(0, stacked(v[0])[1], 0, n_slot)
        s4o[0, span], r4o[1, span], s4o[1, span] = (value[:, g * group : (g + 1) * group] for g in range(3))
        sides[c] = go(
            Flow(s4o.at[0, span], r4o.at[0, span], -1, 0, ("s", 0)),
            Flow(s4o.at[1, span], r4o.at[2, span], 1, 0, ("s", 1)),
        )
        s6[0, 2, part], s6[1, 2, part] = packed(value[:, n_x:])
        value = gather(1, stacked(v[1])[1], 0, n_x)
        loc6[span] = value[:, group : 2 * group]
        for q in range(2):
            rows_q = slice(q * (count // 2), (q + 1) * (count // 2))
            s6[0, q, part], s6[1, q, part] = value[rows_q, :group], value[rows_q, 2 * group :]

    def leave(c):
        span = pl.ds(*cuts[c])
        wait(sides[c])
        sixth[c] = go(Flow(r4o.at[:, span], r4x.at[:, span], 0, 1))

    def spare(c):
        lo, count = cuts[c]
        part = pl.ds(lo // 2, count // 2)
        fourth[c] = go(*[
            Flow(s6.at[k, :, part], r6.at[k, :, part], 2 * k - 1, 0, ("n", k)) for k in range(2)
        ])

    def relay(c):
        lo, count = cuts[c]
        part = pl.ds(lo // 2, count // 2)
        wait(whole[c])
        s5[0, part], s5[1, part] = packed(gather(0, stacked(v_r[pl.ds(lo, count)])[1], n_x, group))
        fifth[c] = go(*[Flow(s5.at[k, part], r5.at[k, part], 2 * k - 1, 0, ("c", k)) for k in range(2)])

    def finish(q, c, stages=(0, 1)):
        lo, count = cuts[c]
        span, part = pl.ds(lo, count), pl.ds(lo // 2, count // 2)
        place = theirs(lo, count) if q else mine(lo, count)
        if 0 in stages:
            wait(fifth[c] if q else fourth[c])
            last = unpacked(r5[0, part], r5[1, part]) if q else unpacked(r6[0, 2, part], r6[1, 2, part])
            main = v_r[span] if q else vacc[0, span]
        if 1 in stages and q:
            wait(sixth[c])
            outer = [r4x[g, span] for g in range(3)]
        elif 1 in stages:
            outer = [jnp.concatenate([r6[k, 0, part], r6[k, 1, part]], axis=0) for k in range(2)]
            outer.insert(1, loc6[span])
        if len(stages) == 2:
            both = stacked(jnp.concatenate([main, *outer, last], axis=1))
            out_t[place] = apply_nt(both, imat, 0, extent)
        elif 0 in stages:
            out_t[place] = apply_nt(stacked(main), imat, 0, n_own) + apply_nt(stacked(last), imat, n_own + n_x, group)
        else:
            both = stacked(jnp.concatenate(outer, axis=1))
            out_t[place] = out_t[place] + apply_nt(both, imat, n_own, n_x)

    stores = []

    def ready(r):
        return max([c for c in range(n) if half + cuts[c][0] < (r + 1) * tile], default=-1)

    def store(c):
        for r in range(feat // tile):
            if ready(r) == c:
                block = far * r + tx * (feat // tile - 1 - r)
                span = pl.ds(pl.multiple_of(block * tile, tile), tile)
                live = lax.broadcasted_iota(jnp.int32, (rows, tile), 0) < limit
                out_v[r] = jnp.where(live, out_t[span].T, 0.0)
                stores.append(pltpu.make_async_copy(out_v.at[r], out_ref.at[:, span], store_sem.at[r]))
                stores[-1].start()

    for step in range(n + 3):
        for stage, lag in ((leave, 3), (forward, 2), (middle, 1), (adjoint, 0)):
            if 0 <= step - lag < n:
                stage(step - lag)
        if step == n + 1:
            for c in range(n - 2):
                relay(c)
                finish(0, c)
        if 0 <= step - 2 < n:
            spare(step - 2)
    relay(n - 2)
    finish(0, n - 2)
    for c in range(n - 2):
        finish(1, c)
    relay(n - 1)
    finish(0, n - 1)
    for c in range(-1, n - 2):
        store(c)
    finish(1, n - 2)
    store(n - 2)
    finish(1, n - 1, (0,))
    finish(1, n - 1, (1,))
    store(n - 1)
    for _, item in tags.values():
        item.sent()
    for item in stores:
        item.wait()


def split(total, parts):
    unit = total // 16
    sizes = [16 * (unit // parts + (1 if k < unit % parts else 0)) for k in range(parts)]
    starts = [sum(sizes[:k]) for k in range(parts)]
    return tuple(zip(starts, sizes))


def pair_call(n_ty, ctrl, interp_wt, interp_cols, conv_wt, conv_cols, halo_index, valid):
    rows, feat = ctrl.shape[2:]
    n_own = conv_wt.shape[2] * conv_wt.shape[3]
    n_slot = halo_index.shape[2] * halo_index.shape[3]
    extent, group, half = n_own + n_slot, n_slot // 4, feat // 2
    cuts = split(half, 4)
    pin = functools.partial(pltpu.with_memory_space_constraint, memory_space=pltpu.HBM)
    hbm = pl.BlockSpec(memory_space=pltpu.HBM)
    vmem = pl.BlockSpec(memory_space=pltpu.VMEM)

    def f32(*shape):
        return pltpu.VMEM(shape, F32)

    def bf16(*shape):
        return pltpu.VMEM(shape, BF16)

    scratch = [
        *[pltpu.VMEM(item.shape[2:], jnp.int32) for item in (interp_cols, conv_cols, halo_index)],
        f32(rows, feat), f32(*interp_wt.shape[2:]), f32(*conv_wt.shape[2:]), f32(*conv_wt.shape[2:]),
        pltpu.VMEM(conv_cols.shape[2:], jnp.int32), pltpu.VMEM(halo_index.shape[2:], jnp.int32),
        bf16(2, feat, rows), bf16(2, rows, extent), bf16(2, 2, n_own, extent), bf16(2, n_own, n_slot),
        f32(feat, n_own), f32(2, 3, half, group), f32(3, 3, half, group),
        f32(half, n_own), f32(3, half, group), f32(2, half, n_own),
        f32(2, 3, half, group), f32(2, 3, half, group), f32(2, half, group),
        f32(2, 3, half, group), f32(2, 3, half, group), f32(2, half, group), f32(2, half, n_own),
        f32(2, half, group), f32(3, half, group), f32(3, half, group), f32(half, n_own),
        f32(2, 3, half // 2, group), f32(2, 3, half // 2, group), f32(half, group),
        f32(2, half // 2, group), f32(2, half // 2, group),
        f32(feat, rows), f32(feat // 128, rows, 128),
    ]
    dma = pltpu.SemaphoreType.DMA
    scratch += [dma((15 + 4 * len(cuts),)), dma((5 + 14 * len(cuts),)), dma((6,)), dma((feat // 128,))]
    return pl.pallas_call(
        functools.partial(pair_kernel, n_ty, cuts),
        out_shape=jax.ShapeDtypeStruct((rows, feat), F32),
        in_specs=[pl.BlockSpec(memory_space=pltpu.SMEM)] + [hbm] * 6,
        out_specs=pl.BlockSpec(memory_space=pl.ANY),
        scratch_shapes=scratch,
        compiler_params=pltpu.CompilerParams(
            collective_id=0, has_side_effects=True, vmem_limit_bytes=52 * 1024 * 1024
        ),
    )(
        valid, pin(ctrl[0, 0]), pin(interp_wt[0, 0]), pin(interp_cols[0, 0]), pin(conv_wt[0, 0]),
        pin(conv_cols[0, 0]), pin(halo_index[0, 0]),
    )


def pairs_fit(n_tx, ctrl, halo_index):
    slot = halo_index.shape[3]
    return n_tx == 2 and halo_index.shape[2] == 8 and slot == 64 and ctrl.shape[3] % 128 == 0


def solution(mesh):
    n_ty, n_tx = mesh.shape["ty"], mesh.shape["tx"]

    def body(ctrl, interp_wt, interp_cols, conv_wt, conv_cols, halo_index, valid):
        rows, feat = ctrl.shape[2:]
        n_own = conv_wt.shape[2] * conv_wt.shape[3]
        n_slot = halo_index.shape[2] * halo_index.shape[3]
        extent = n_own + n_slot
        if pairs_fit(n_tx, ctrl, halo_index) and rows == n_own:
            args = ctrl, interp_wt, interp_cols, conv_wt, conv_cols, halo_index, valid
            return pair_call(n_ty, *args)[None, None]
        tiles = feat // 128
        first = 128 * max(tiles - tiles // 2, 1)
        chunks = ((0, first), (first, feat - first)) if feat > first else ((0, feat),)
        widths = [width for _, width in chunks]
        pin = functools.partial(pltpu.with_memory_space_constraint, memory_space=pltpu.HBM)
        hbm = pl.BlockSpec(memory_space=pltpu.HBM)
        vmem = pl.BlockSpec(memory_space=pltpu.VMEM)
        scratch = [
            pltpu.VMEM(interp_wt.shape[2:], F32),
            pltpu.VMEM(conv_wt.shape[2:], F32),
            pltpu.VMEM((2, rows, extent), BF16),
            pltpu.VMEM((2, extent, rows), BF16),
            pltpu.VMEM((2, n_own, extent), BF16),
            pltpu.VMEM((2, extent, n_own), BF16),
            pltpu.VMEM((n_slot, n_own), BF16),
            pltpu.VMEM((n_own, n_slot), BF16),
        ]
        assert rows == n_own
        scratch += [pltpu.VMEM((n_own, width), F32) for width in widths]
        scratch += [pltpu.VMEM((2, extent, width), BF16) for width in widths]
        scratch += [pltpu.VMEM((n_slot, width), F32) for _ in range(8) for width in widths]
        scratch += [pltpu.SemaphoreType.DMA((4, len(chunks), 8))] * 2
        scratch += [pltpu.SemaphoreType.DMA((2 + len(chunks),)), pltpu.SemaphoreType.DMA((len(chunks),))]
        out = pl.pallas_call(
            functools.partial(kernel, n_ty, n_tx, chunks),
            out_shape=jax.ShapeDtypeStruct((rows, feat), F32),
            in_specs=[pl.BlockSpec(memory_space=pltpu.SMEM), hbm, hbm, vmem, hbm, vmem, vmem],
            out_specs=pl.BlockSpec(memory_space=pl.ANY),
            scratch_shapes=scratch,
            compiler_params=pltpu.CompilerParams(
                collective_id=0, has_side_effects=True, vmem_limit_bytes=44 * 1024 * 1024
            ),
        )(
            valid, pin(ctrl[0, 0]), pin(interp_wt[0, 0]), pin(interp_cols[0, 0]), pin(conv_wt[0, 0]),
            pin(conv_cols[0, 0]), pin(halo_index[0, 0]),
        )
        return out[None, None]

    placed = (
        P("ty", "tx", None, None),
        P("ty", "tx", None, None, None),
        P("ty", "tx", None, None),
        P("ty", "tx", None, None, None),
        P("ty", "tx", None, None),
        P("ty", "tx", None, None),
        P("ty", "tx"),
    )
    return jax.shard_map(
        body, mesh=mesh, in_specs=placed, out_specs=P("ty", "tx", None, None), check_vma=False
    )
```

```python
import functools

import jax
import jax.numpy as jnp
from jax import lax
from jax.experimental import pallas as pl
from jax.experimental.pallas import tpu as pltpu
from jax.sharding import PartitionSpec as P

MESH = pl.DeviceIdType.MESH
DIRECTIONS = ((-1, -1), (-1, 0), (-1, 1), (0, -1), (0, 1), (1, -1), (1, 0), (1, 1))
ORDER = (0, 2, 5, 7, 3, 4, 1, 6)
F32, BF16 = jnp.float32, jnp.bfloat16


def halves(x):
    hi = x.astype(BF16)
    return hi, (x - hi.astype(F32)).astype(BF16)


def dot(a, b):
    return jnp.dot(a, b, preferred_element_type=F32)


def dot_nt(a, b):
    return lax.dot_general(a, b, (((1,), (1,)), ((), ())), preferred_element_type=F32)


def kernel(
    n_ty, n_tx, chunks, valid_ref, ctrl_hbm, iwt_hbm, icols_ref, cwt_hbm, ccols_ref, halo_ref,
    out_ref, iwt_ref, cwt_ref, imat, imat_t, cmat, cmat_t, pick, pick_t, *rest,
):
    n_chunks = len(chunks)
    send_sem, recv_sem, load_sem, store_sem = rest[-4:]
    buffers = rest[:-4]
    own = buffers[:n_chunks]
    rhs = buffers[n_chunks : 2 * n_chunks]
    send = [buffers[(2 + e) * n_chunks : (3 + e) * n_chunks] for e in range(4)]
    recv = [buffers[(6 + e) * n_chunks : (7 + e) * n_chunks] for e in range(4)]
    loads = [pltpu.make_async_copy(iwt_hbm, iwt_ref, load_sem.at[0])]
    for c, (lo, width) in enumerate(chunks):
        loads.append(
            pltpu.make_async_copy(ctrl_hbm.at[:, lo : lo + width], own[c], load_sem.at[1 + c])
        )
    loads.append(pltpu.make_async_copy(cwt_hbm, cwt_ref, load_sem.at[1 + n_chunks]))
    for item in loads:
        item.start()
    ty, tx = lax.axis_index("ty"), lax.axis_index("tx")
    rows = out_ref.shape[0]
    n_own = own[0].shape[0]
    n_slot = recv[0][0].shape[0]
    slot = n_slot // 8
    extent = n_own + n_slot

    def there(off):
        return jnp.logical_and(ty + off >= 0, ty + off < n_ty)

    def peer(row_off, col_off):
        return ty + row_off, lax.rem(tx + col_off + n_tx, n_tx)

    barrier = pltpu.get_barrier_semaphore()
    for row_off, col_off in DIRECTIONS:
        @pl.when(there(row_off))
        def _():
            pl.semaphore_signal(
                barrier, inc=1, device_id=peer(row_off, col_off), device_id_type=MESH
            )

    def copy(e, c, d):
        sign = -1 if e < 2 else 1
        row_off, col_off = DIRECTIONS[d]
        piece = pl.ds(d * slot, slot)
        return pltpu.make_async_remote_copy(
            src_ref=send[e][c].at[piece],
            dst_ref=recv[e][c].at[piece],
            send_sem=send_sem.at[e, c, d],
            recv_sem=recv_sem.at[e, c, d],
            device_id=peer(sign * row_off, sign * col_off),
            device_id_type=MESH,
        )

    def each(e, c, sending, action):
        sign = -1 if e < 2 else 1
        for d in ORDER:
            row_off = DIRECTIONS[d][0] * (sign if sending else -sign)
            if row_off == 0:
                action(copy(e, c, d))
            else:
                pl.when(there(row_off))(functools.partial(lambda e, c, d: action(copy(e, c, d)), e, c, d))

    def start(e, c):
        each(e, c, True, lambda item: item.start())

    def arrived(e, c):
        each(e, c, False, lambda item: item.wait_recv())

    def spread(wt_ref, cols_ref, mat, mat_t, base=0, count=extent):
        blocks, height, width = wt_ref.shape
        for b in range(blocks):
            index = cols_ref[b : b + 1, :]
            place_of = lax.broadcasted_iota(jnp.int32, (count, width), 0) + base
            hot = (place_of == index).astype(F32).astype(BF16)
            hi, lo = halves(wt_ref[b])
            span = pl.ds(b * height, height)
            if mat is not None:
                mat[0, span], mat[1, span] = halves(dot_nt(hi, hot) + dot_nt(lo, hot))
            if mat_t is not None:
                part = pl.ds(base, count)
                mat_t[0, part, span], mat_t[1, part, span] = halves(dot_nt(hot, hi) + dot_nt(hot, lo))

    def product(mat, row0, count, col0, depth, c, base):
        a_hi = mat[0, row0 : row0 + count, col0 : col0 + depth]
        a_lo = mat[1, row0 : row0 + count, col0 : col0 + depth]
        b_hi, b_lo = rhs[c][0, base : base + depth], rhs[c][1, base : base + depth]
        return dot(a_hi, b_hi) + (dot(a_hi, b_lo) + dot(a_lo, b_hi))

    def gathered(e, c):
        hi, lo = halves(recv[e][c][...])
        return dot(pick_t[...], hi) + dot(pick_t[...], lo)

    def place(c, base, value):
        rhs[c][0, base : base + value.shape[0]], rhs[c][1, base : base + value.shape[0]] = halves(value)

    def picked(c):
        return dot(pick[...], rhs[c][0, :n_own]) + dot(pick[...], rhs[c][1, :n_own])

    for e in range(4):
        sign = -1 if e < 2 else 1
        for d, (row_off, _) in enumerate(DIRECTIONS):
            if row_off:
                @pl.when(jnp.logical_not(there(-sign * row_off)))
                def _():
                    for c in range(n_chunks):
                        piece = recv[e][c].at[pl.ds(d * slot, slot)]
                        piece[...] = jnp.zeros(piece.shape, F32)

    loads[0].wait()
    spread(iwt_ref, icols_ref, None, imat_t, n_own, n_slot)
    limit = valid_ref[0, 0]
    edge = jnp.int32(2)
    edge += jnp.where(there(-1), 3, 0) + jnp.where(there(1), 3, 0)
    pl.semaphore_wait(barrier, edge)

    def keep(width):
        return lax.broadcasted_iota(jnp.int32, (rows, width), 0) < limit

    for c, (lo, width) in enumerate(chunks):
        loads[1 + c].wait()
        place(c, 0, jnp.where(keep(width), own[c][...], 0.0))
        send[0][c][...] = product(imat_t, n_own, n_slot, 0, rows, c, 0)
        start(0, c)
    spread(iwt_ref, icols_ref, None, imat_t, 0, n_own)
    for c in range(n_chunks):
        own[c][...] = product(imat_t, 0, n_own, 0, rows, c, 0)
    halo = jnp.concatenate([halo_ref[d : d + 1, :] for d in range(8)], axis=1)
    hot = (lax.broadcasted_iota(jnp.int32, (n_own, n_slot), 0) == halo).astype(F32)
    loads[-1].wait()
    pick_t[...] = hot.astype(BF16)
    pick[...] = hot.T.astype(BF16)
    spread(cwt_ref, ccols_ref, None, cmat_t)
    for c in range(n_chunks):
        arrived(0, c)
        place(c, 0, own[c][...] + gathered(0, c))
        send[1][c][...] = product(cmat_t, n_own, n_slot, 0, n_own, c, 0)
        start(1, c)
        own[c][...] = product(cmat_t, 0, n_own, 0, n_own, c, 0)
    spread(cwt_ref, ccols_ref, cmat, None)
    spread(iwt_ref, icols_ref, imat, None)
    for c in range(n_chunks):
        arrived(1, c)
        place(c, 0, own[c][...] + gathered(1, c))
        send[2][c][...] = picked(c)
        start(2, c)
        own[c][...] = product(cmat, 0, n_own, 0, n_own, c, 0)
    for c in range(n_chunks):
        arrived(2, c)
        place(c, n_own, recv[2][c][...])
        place(c, 0, own[c][...] + product(cmat, 0, n_own, n_own, n_slot, c, n_own))
        send[3][c][...] = picked(c)
        start(3, c)
        own[c][...] = product(imat, 0, rows, 0, n_own, c, 0)
    stores = []
    for c, (lo, width) in enumerate(chunks):
        arrived(3, c)
        place(c, n_own, recv[3][c][...])
        total = own[c][...] + product(imat, 0, rows, n_own, n_slot, c, n_own)
        own[c][...] = jnp.where(keep(width), total, 0.0)
        stores.append(
            pltpu.make_async_copy(own[c], out_ref.at[:, lo : lo + width], store_sem.at[c])
        )
        stores[c].start()
    for e in range(4):
        for c in range(n_chunks):
            each(e, c, True, lambda item: item.wait_send())
    for item in stores:
        item.wait()

OWN_ORDER = (0, 2, 3, 4, 5, 7, 1, 6)
FAR_ORDER = (0, 2, 3, 4, 5, 7, 6, 1)


def stacked(x):
    hi, lo = halves(x)
    return hi, jnp.concatenate([hi, lo], axis=0)


def folded(x):
    half = x.shape[0] // 2
    return x[:half] + x[half:]


def pair_kernel(
    n_ty, cuts, valid_ref, ctrl_hbm, iwt_hbm, icols_hbm, cwt_hbm, ccols_hbm, halo_hbm,
    out_ref, icols_ref, ccols_ref, halo_ref, ctrl, iwt, cwt, cwt_f, ccols_f, halo_f, xt, imat, imat_t, cmat, cmat_t, pick, pick_t,
    zp, s1, near, zf, r1o, bown, s2, r2, loc2, s3, r3, loc3, vacc,
    s4o, r4o, r4x, v_r, s6, r6, loc6, s5, r5, out_t, out_v, send_sem, recv_sem, load_sem, store_sem,
):
    rows, feat = ctrl.shape
    half = feat // 2
    n_own, n_slot = pick.shape[1:]
    slot, group = n_slot // 8, n_slot // 4
    extent = n_own + n_slot
    n_x = 3 * group
    blocks = cwt.shape[0]
    ty, tx = lax.axis_index("ty"), lax.axis_index("tx")
    far = 1 - tx

    loads = [
        pltpu.make_async_copy(cwt_hbm, cwt, load_sem.at[0]),
        pltpu.make_async_copy(iwt_hbm, iwt, load_sem.at[1]),
        pltpu.make_async_copy(ctrl_hbm, ctrl, load_sem.at[2]),
        pltpu.make_async_copy(icols_hbm, icols_ref, load_sem.at[3]),
        pltpu.make_async_copy(ccols_hbm, ccols_ref, load_sem.at[4]),
        pltpu.make_async_copy(halo_hbm, halo_ref, load_sem.at[5]),
    ]
    for item in loads:
        item.start()

    def there(off):
        return jnp.logical_and(ty + off >= 0, ty + off < n_ty)

    barrier = pltpu.get_barrier_semaphore()
    partners = [(0, 1), (-1, 0), (1, 0)]
    for row_off, flip in partners:
        def greet(row_off=row_off, flip=flip):
            pl.semaphore_signal(
                barrier, inc=1, device_id=(ty + row_off, far if flip else tx), device_id_type=MESH
            )
        if row_off:
            pl.when(there(row_off))(greet)
        else:
            greet()

    flows, tags = [], {}

    class Flow:
        def __init__(self, src, dst, row_off, flip, tag=None):
            self.row_off = row_off
            self.tag = tag or len(flows)
            key = tags.setdefault(self.tag, [len(tags), None])[0]
            self.copy = pltpu.make_async_remote_copy(
                src_ref=src, dst_ref=dst, send_sem=send_sem.at[key], recv_sem=recv_sem.at[len(flows)],
                device_id=(ty + row_off, far if flip else tx), device_id_type=MESH,
            )
            flows.append(self)

        def act(self, sign, action):
            if self.row_off:
                pl.when(there(sign * self.row_off))(action)
            else:
                action()

        def start(self):
            before = tags[self.tag][1]
            if before is not None:
                before.sent()
            tags[self.tag][1] = self
            self.act(1, lambda: self.copy.start())

        def arrived(self):
            self.act(-1, lambda: self.copy.wait_recv())

        def sent(self):
            self.act(1, lambda: self.copy.wait_send())

    def go(*items):
        for item in items:
            item.start()
        return list(items)

    def wait(items):
        for item in items:
            item.arrived()

    def lane(count, width=group):
        return lax.broadcasted_iota(jnp.int32, (count, width), 1)

    def blend(first, second):
        return jnp.where(lane(first.shape[0]) < slot, first, second)

    def packed(x):
        top, low = x[: x.shape[0] // 2], x[x.shape[0] // 2 :]
        low = pltpu.roll(low, slot, 1)
        return blend(top, low), blend(low, top)

    def unpacked(first, second):
        low = pltpu.roll(blend(second, first), slot, 1)
        return jnp.concatenate([blend(first, second), low], axis=0)

    def dense(mat, mat_t, b, weights, index, order):
        where = index
        for place, d in enumerate(order):
            low = n_own + d * slot
            inside = jnp.logical_and(index >= low, index < low + slot)
            where = jnp.where(inside, index + (place - d) * slot, where)
        height, width = weights.shape
        hot = lax.broadcasted_iota(jnp.int32, (extent, width), 0) == where
        _, both = stacked(weights)
        span = pl.ds(b * height, height)
        hot = hot.astype(F32).astype(BF16)
        mat[0, span], mat[1, span] = halves(folded(dot_nt(both, hot)))
        turned = dot_nt(hot, both)
        mat_t[0, :, span], mat_t[1, :, span] = halves(turned[:, :height] + turned[:, height:])

    def choose(t, ref, order):
        halo = jnp.concatenate([ref[d : d + 1, :] for d in order], axis=1)
        hot = lax.broadcasted_iota(jnp.int32, (n_own, n_slot), 0) == halo
        hot = hot.astype(F32)
        pick[t], pick_t[t] = hot.astype(BF16), hot.T.astype(BF16)

    def scatter(t, pieces, lo=0):
        value = jnp.concatenate(pieces, axis=1) if len(pieces) > 1 else pieces[0]
        return folded(dot(stacked(value)[1], pick_t[t, lo : lo + value.shape[1]]))

    def apply(x, mat, lo, count):
        hi, both = x
        return folded(dot(both, mat[0, :, lo : lo + count])) + dot(hi, mat[1, :, lo : lo + count])

    def apply_t(x, mat, lo, count):
        hi, both = x
        return folded(dot(both, mat[0, lo : lo + count])) + dot(hi, mat[1, lo : lo + count])

    def gather(t, both, lo, count):
        return folded(dot(both, pick[t, :, lo : lo + count]))

    def within(side, lo, count):
        start = side * lo + (1 - side) * (half - lo - count)
        return pl.ds(pl.multiple_of(start, 16), count)

    def placed(side, lo, count):
        start = side * (half + lo) + (1 - side) * (half - lo - count)
        return pl.ds(pl.multiple_of(start, 16), count)

    def mine(lo, count):
        return placed(tx, lo, count)

    def theirs(lo, count):
        return placed(far, lo, count)

    def blank(ref):
        ref[...] = jnp.zeros(ref.shape, ref.dtype)

    @pl.when(jnp.logical_not(there(-1)))
    def _():
        for ref in (near.at[0], r2.at[0], r3.at[1], r4o.at[2], r6.at[1], r5.at[1]):
            blank(ref)

    @pl.when(jnp.logical_not(there(1)))
    def _():
        for ref in (near.at[2], r2.at[1], r3.at[0], r4o.at[0], r6.at[0], r5.at[0]):
            blank(ref)

    loads[0].wait()
    pl.semaphore_wait(barrier, 1 + jnp.where(there(-1), 1, 0) + jnp.where(there(1), 1, 0))
    for item in loads[3:]:
        item.wait()
    tables = go(Flow(ccols_ref, ccols_f, 0, 1), Flow(halo_ref, halo_f, 0, 1))
    weights = go(Flow(cwt, cwt_f, 0, 1))

    limit = valid_ref[0, 0]
    loads[1].wait()
    for b in range(iwt.shape[0]):
        dense(imat, imat_t, b, iwt[b], icols_ref[b : b + 1, :], OWN_ORDER)
    loads[2].wait()
    tile = 128
    for lo in range(0, feat, tile):
        live = lax.broadcasted_iota(jnp.int32, (rows, tile), 0) < limit
        piece = jnp.where(live, ctrl[:, lo : lo + tile], 0.0).T
        xt[0, lo : lo + tile], xt[1, lo : lo + tile] = halves(piece)
    last = []
    for q in range(2):
        span = slice(q * half, (q + 1) * half)
        both = jnp.concatenate([xt[0, span], xt[1, span]], axis=0)
        value = apply((xt[0, span], both), imat, n_own, n_slot)
        s1[0, q], near[1, q], s1[1, q] = (value[:, g * group : (g + 1) * group] for g in range(3))
        last.append(value[:, n_x:])
    s1[0, 2], s1[1, 2] = packed(jnp.concatenate(last, axis=0))
    first = go(Flow(s1.at[0], near.at[0], 1, 0), Flow(s1.at[1], near.at[2], -1, 0))
    for q in range(2):
        span = slice(q * half, (q + 1) * half)
        both = jnp.concatenate([xt[0, span], xt[1, span]], axis=0)
        zp[span] = apply((xt[0, span], both), imat, 0, n_own)
    choose(0, halo_ref, OWN_ORDER)
    wait(first)
    extra = unpacked(near[0, 2], near[2, 2])
    for q in range(2):
        span = slice(q * half, (q + 1) * half)
        zp[span] = zp[span] + scatter(0, [extra[span]], n_x)
    crossed = []
    for lo, count in cuts:
        span = pl.ds(lo, count)
        crossed.append(go(
            Flow(zp.at[theirs(lo, count)], zf.at[span], 0, 1),
            Flow(near.at[:, far, within(far, lo, count)], r1o.at[:, span], 0, 1),
        ))
    for b in range(blocks):
        dense(cmat.at[0], cmat_t.at[0], b, cwt[b], ccols_ref[b : b + 1, :], OWN_ORDER)
    wait(tables)
    choose(1, halo_f, FAR_ORDER)
    wait(weights)
    for b in range(blocks):
        dense(cmat.at[1], cmat_t.at[1], b, cwt_f[b], ccols_f[b : b + 1, :], FAR_ORDER)

    second, third, fourth, fifth, sixth, sides, whole = {}, {}, {}, {}, {}, {}, {}
    n = len(cuts)

    def swap(c, sent, got, kept, sign, tag, value):
        span = pl.ds(*cuts[c])
        last = []
        for t in range(2):
            sent[0, t, span], kept[t, span] = value[t][:, :group], value[t][:, group : 2 * group]
            sent[1, t, span] = value[t][:, 2 * group : n_x]
            last.append(value[t][:, n_x:])
        sent[0, 2, span], sent[1, 2, span] = blend(last[0], last[1]), blend(last[1], last[0])
        return go(*[
            Flow(sent.at[k, :, span], got.at[k, :, span], sign - 2 * k * sign, 0, (tag, k)) for k in range(2)
        ])

    def swapped(c, got, kept):
        span = pl.ds(*cuts[c])
        return [
            jnp.concatenate([
                got[0, 1 - t, span], kept[1 - t, span], got[1, 1 - t, span],
                blend(got[t, 2, span], got[1 - t, 2, span]),
            ], axis=1)
            for t in range(2)
        ]

    def adjoint(c):
        lo, count = cuts[c]
        span = pl.ds(lo, count)
        here = within(tx, lo, count)
        wait(crossed[c])
        z = [
            zp[mine(lo, count)] + scatter(0, [r1o[g, span] for g in range(3)]),
            zf[span] + scatter(1, [near[g, tx, here] for g in range(3)]),
        ]
        z = [stacked(item) for item in z]
        second[c] = swap(c, s2, r2, loc2, 1, "b", [apply(z[t], cmat.at[t], n_own, n_slot) for t in range(2)])
        for t in range(2):
            bown[t, span] = apply(z[t], cmat.at[t], 0, n_own)

    def middle(c):
        span = pl.ds(*cuts[c])
        wait(second[c])
        slots = swapped(c, r2, loc2)
        w = [stacked(bown[t, span] + scatter(t, [slots[t]])) for t in range(2)]
        third[c] = swap(c, s3, r3, loc3, -1, "w", [gather(t, w[t][1], 0, n_slot) for t in range(2)])
        for t in range(2):
            vacc[t, span] = apply_t(w[t], cmat_t.at[t], 0, n_own)

    def forward(c):
        lo, count = cuts[c]
        span, part = pl.ds(lo, count), pl.ds(lo // 2, count // 2)
        wait(third[c])
        slots = swapped(c, r3, loc3)
        v = [None, None]
        for t in (1, 0):
            v[t] = vacc[t, span] + apply_t(stacked(slots[t]), cmat_t.at[t], n_own, n_slot)
            vacc[t, span] = v[t]
            if t:
                whole[c] = go(Flow(vacc.at[1, span], v_r.at[span], 0, 1))
        value = gather(0, stacked(v[0])[1], 0, n_slot)
        s4o[0, span], r4o[1, span], s4o[1, span] = (value[:, g * group : (g + 1) * group] for g in range(3))
        sides[c] = go(
            Flow(s4o.at[0, span], r4o.at[0, span], -1, 0, ("s", 0)),
            Flow(s4o.at[1, span], r4o.at[2, span], 1, 0, ("s", 1)),
        )
        s6[0, 2, part], s6[1, 2, part] = packed(value[:, n_x:])
        value = gather(1, stacked(v[1])[1], 0, n_x)
        loc6[span] = value[:, group : 2 * group]
        for q in range(2):
            rows_q = slice(q * (count // 2), (q + 1) * (count // 2))
            s6[0, q, part], s6[1, q, part] = value[rows_q, :group], value[rows_q, 2 * group :]

    def leave(c):
        span = pl.ds(*cuts[c])
        wait(sides[c])
        sixth[c] = go(Flow(r4o.at[:, span], r4x.at[:, span], 0, 1))

    def spare(c):
        lo, count = cuts[c]
        part = pl.ds(lo // 2, count // 2)
        fourth[c] = go(*[
            Flow(s6.at[k, :, part], r6.at[k, :, part], 2 * k - 1, 0) for k in range(2)
        ])

    def relay(c):
        lo, count = cuts[c]
        part = pl.ds(lo // 2, count // 2)
        wait(whole[c])
        s5[0, part], s5[1, part] = packed(gather(0, stacked(v_r[pl.ds(lo, count)])[1], n_x, group))
        fifth[c] = go(*[Flow(s5.at[k, part], r5.at[k, part], 2 * k - 1, 0) for k in range(2)])

    def finish(q, c, stages=(0, 1)):
        lo, count = cuts[c]
        span, part = pl.ds(lo, count), pl.ds(lo // 2, count // 2)
        place = theirs(lo, count) if q else mine(lo, count)
        if 0 in stages:
            wait(fifth[c] if q else fourth[c])
            last = unpacked(r5[0, part], r5[1, part]) if q else unpacked(r6[0, 2, part], r6[1, 2, part])
            main = v_r[span] if q else vacc[0, span]
        if 1 in stages and q:
            wait(sixth[c])
            outer = [r4x[g, span] for g in range(3)]
        elif 1 in stages:
            outer = [jnp.concatenate([r6[k, 0, part], r6[k, 1, part]], axis=0) for k in range(2)]
            outer.insert(1, loc6[span])
        if len(stages) == 2:
            both = stacked(jnp.concatenate([main, *outer, last], axis=1))
            out_t[place] = apply_t(both, imat_t, 0, extent)
        elif 0 in stages:
            out_t[place] = apply_t(stacked(main), imat_t, 0, n_own) + apply_t(stacked(last), imat_t, n_own + n_x, group)
        else:
            both = stacked(jnp.concatenate(outer, axis=1))
            out_t[place] = out_t[place] + apply_t(both, imat_t, n_own, n_x)

    stores = []

    def ready(r):
        return max([c for c in range(n) if half + cuts[c][0] < (r + 1) * tile], default=-1)

    def store(c):
        for r in range(feat // tile):
            if ready(r) == c:
                block = far * r + tx * (feat // tile - 1 - r)
                span = pl.ds(pl.multiple_of(block * tile, tile), tile)
                live = lax.broadcasted_iota(jnp.int32, (rows, tile), 0) < limit
                out_v[r] = jnp.where(live, out_t[span].T, 0.0)
                stores.append(pltpu.make_async_copy(out_v.at[r], out_ref.at[:, span], store_sem.at[r]))
                stores[-1].start()

    for step in range(n + 3):
        for stage, lag in ((adjoint, 0), (middle, 1), (forward, 2), (leave, 3)):
            if 0 <= step - lag < n:
                stage(step - lag)
        if step == n:
            for c in range(n - 2):
                spare(c)
        if step == n + 1:
            for c in range(n - 2):
                relay(c)
            spare(n - 2)
            spare(n - 1)
            for c in range(n - 2):
                finish(0, c)
    relay(n - 2)
    finish(0, n - 2)
    for c in range(n - 2):
        finish(1, c)
    finish(0, n - 1)
    relay(n - 1)
    for c in range(-1, n - 2):
        store(c)
    finish(1, n - 2)
    store(n - 2)
    finish(1, n - 1, (0,))
    finish(1, n - 1, (1,))
    store(n - 1)
    for _, item in tags.values():
        item.sent()
    for item in stores:
        item.wait()


def split(total, parts):
    unit = total // 16
    sizes = [16 * (unit // parts + (1 if k < unit % parts else 0)) for k in range(parts)]
    starts = [sum(sizes[:k]) for k in range(parts)]
    return tuple(zip(starts, sizes))


def pair_call(n_ty, ctrl, interp_wt, interp_cols, conv_wt, conv_cols, halo_index, valid):
    rows, feat = ctrl.shape[2:]
    n_own = conv_wt.shape[2] * conv_wt.shape[3]
    n_slot = halo_index.shape[2] * halo_index.shape[3]
    extent, group, half = n_own + n_slot, n_slot // 4, feat // 2
    cuts = split(half, 4)
    pin = functools.partial(pltpu.with_memory_space_constraint, memory_space=pltpu.HBM)
    hbm = pl.BlockSpec(memory_space=pltpu.HBM)
    vmem = pl.BlockSpec(memory_space=pltpu.VMEM)

    def f32(*shape):
        return pltpu.VMEM(shape, F32)

    def bf16(*shape):
        return pltpu.VMEM(shape, BF16)

    scratch = [
        *[pltpu.VMEM(item.shape[2:], jnp.int32) for item in (interp_cols, conv_cols, halo_index)],
        f32(rows, feat), f32(*interp_wt.shape[2:]), f32(*conv_wt.shape[2:]), f32(*conv_wt.shape[2:]),
        pltpu.VMEM(conv_cols.shape[2:], jnp.int32), pltpu.VMEM(halo_index.shape[2:], jnp.int32),
        bf16(2, feat, rows), bf16(2, rows, extent), bf16(2, extent, rows),
        bf16(2, 2, n_own, extent), bf16(2, 2, extent, n_own), bf16(2, n_own, n_slot), bf16(2, n_slot, n_own),
        f32(feat, n_own), f32(2, 3, half, group), f32(3, 3, half, group),
        f32(half, n_own), f32(3, half, group), f32(2, half, n_own),
        f32(2, 3, half, group), f32(2, 3, half, group), f32(2, half, group),
        f32(2, 3, half, group), f32(2, 3, half, group), f32(2, half, group), f32(2, half, n_own),
        f32(2, half, group), f32(3, half, group), f32(3, half, group), f32(half, n_own),
        f32(2, 3, half // 2, group), f32(2, 3, half // 2, group), f32(half, group),
        f32(2, half // 2, group), f32(2, half // 2, group),
        f32(feat, rows), f32(feat // 128, rows, 128),
    ]
    dma = pltpu.SemaphoreType.DMA
    scratch += [dma((11 + 8 * len(cuts),)), dma((5 + 14 * len(cuts),)), dma((6,)), dma((feat // 128,))]
    return pl.pallas_call(
        functools.partial(pair_kernel, n_ty, cuts),
        out_shape=jax.ShapeDtypeStruct((rows, feat), F32),
        in_specs=[pl.BlockSpec(memory_space=pltpu.SMEM)] + [hbm] * 6,
        out_specs=pl.BlockSpec(memory_space=pl.ANY),
        scratch_shapes=scratch,
        compiler_params=pltpu.CompilerParams(
            collective_id=0, has_side_effects=True, vmem_limit_bytes=52 * 1024 * 1024
        ),
    )(
        valid, pin(ctrl[0, 0]), pin(interp_wt[0, 0]), pin(interp_cols[0, 0]), pin(conv_wt[0, 0]),
        pin(conv_cols[0, 0]), pin(halo_index[0, 0]),
    )


def pairs_fit(n_tx, ctrl, halo_index):
    slot = halo_index.shape[3]
    return n_tx == 2 and halo_index.shape[2] == 8 and slot == 64 and ctrl.shape[3] % 128 == 0


def solution(mesh):
    n_ty, n_tx = mesh.shape["ty"], mesh.shape["tx"]

    def body(ctrl, interp_wt, interp_cols, conv_wt, conv_cols, halo_index, valid):
        rows, feat = ctrl.shape[2:]
        n_own = conv_wt.shape[2] * conv_wt.shape[3]
        n_slot = halo_index.shape[2] * halo_index.shape[3]
        extent = n_own + n_slot
        if pairs_fit(n_tx, ctrl, halo_index) and rows == n_own:
            args = ctrl, interp_wt, interp_cols, conv_wt, conv_cols, halo_index, valid
            return pair_call(n_ty, *args)[None, None]
        tiles = feat // 128
        first = 128 * max(tiles - tiles // 2, 1)
        chunks = ((0, first), (first, feat - first)) if feat > first else ((0, feat),)
        widths = [width for _, width in chunks]
        pin = functools.partial(pltpu.with_memory_space_constraint, memory_space=pltpu.HBM)
        hbm = pl.BlockSpec(memory_space=pltpu.HBM)
        vmem = pl.BlockSpec(memory_space=pltpu.VMEM)
        scratch = [
            pltpu.VMEM(interp_wt.shape[2:], F32),
            pltpu.VMEM(conv_wt.shape[2:], F32),
            pltpu.VMEM((2, rows, extent), BF16),
            pltpu.VMEM((2, extent, rows), BF16),
            pltpu.VMEM((2, n_own, extent), BF16),
            pltpu.VMEM((2, extent, n_own), BF16),
            pltpu.VMEM((n_slot, n_own), BF16),
            pltpu.VMEM((n_own, n_slot), BF16),
        ]
        assert rows == n_own
        scratch += [pltpu.VMEM((n_own, width), F32) for width in widths]
        scratch += [pltpu.VMEM((2, extent, width), BF16) for width in widths]
        scratch += [pltpu.VMEM((n_slot, width), F32) for _ in range(8) for width in widths]
        scratch += [pltpu.SemaphoreType.DMA((4, len(chunks), 8))] * 2
        scratch += [pltpu.SemaphoreType.DMA((2 + len(chunks),)), pltpu.SemaphoreType.DMA((len(chunks),))]
        out = pl.pallas_call(
            functools.partial(kernel, n_ty, n_tx, chunks),
            out_shape=jax.ShapeDtypeStruct((rows, feat), F32),
            in_specs=[pl.BlockSpec(memory_space=pltpu.SMEM), hbm, hbm, vmem, hbm, vmem, vmem],
            out_specs=pl.BlockSpec(memory_space=pl.ANY),
            scratch_shapes=scratch,
            compiler_params=pltpu.CompilerParams(
                collective_id=0, has_side_effects=True, vmem_limit_bytes=44 * 1024 * 1024
            ),
        )(
            valid, pin(ctrl[0, 0]), pin(interp_wt[0, 0]), pin(interp_cols[0, 0]), pin(conv_wt[0, 0]),
            pin(conv_cols[0, 0]), pin(halo_index[0, 0]),
        )
        return out[None, None]

    placed = (
        P("ty", "tx", None, None),
        P("ty", "tx", None, None, None),
        P("ty", "tx", None, None),
        P("ty", "tx", None, None, None),
        P("ty", "tx", None, None),
        P("ty", "tx", None, None),
        P("ty", "tx"),
    )
    return jax.shard_map(
        body, mesh=mesh, in_specs=placed, out_specs=P("ty", "tx", None, None), check_vma=False
    )
```

```python
import functools

import jax
import jax.numpy as jnp
from jax import lax
from jax.experimental import pallas as pl
from jax.experimental.pallas import tpu as pltpu
from jax.sharding import PartitionSpec as P

MESH = pl.DeviceIdType.MESH
DIRECTIONS = ((-1, -1), (-1, 0), (-1, 1), (0, -1), (0, 1), (1, -1), (1, 0), (1, 1))
ORDER = (0, 2, 5, 7, 3, 4, 1, 6)
F32, BF16 = jnp.float32, jnp.bfloat16


def halves(x):
    hi = x.astype(BF16)
    return hi, (x - hi.astype(F32)).astype(BF16)


def dot(a, b):
    return jnp.dot(a, b, preferred_element_type=F32)


def dot_nt(a, b):
    return lax.dot_general(a, b, (((1,), (1,)), ((), ())), preferred_element_type=F32)


def kernel(
    n_ty, n_tx, chunks, valid_ref, ctrl_hbm, iwt_hbm, icols_ref, cwt_hbm, ccols_ref, halo_ref,
    out_ref, iwt_ref, cwt_ref, imat, imat_t, cmat, cmat_t, pick, pick_t, *rest,
):
    n_chunks = len(chunks)
    send_sem, recv_sem, load_sem, store_sem = rest[-4:]
    buffers = rest[:-4]
    own = buffers[:n_chunks]
    rhs = buffers[n_chunks : 2 * n_chunks]
    send = [buffers[(2 + e) * n_chunks : (3 + e) * n_chunks] for e in range(4)]
    recv = [buffers[(6 + e) * n_chunks : (7 + e) * n_chunks] for e in range(4)]
    loads = [pltpu.make_async_copy(iwt_hbm, iwt_ref, load_sem.at[0])]
    for c, (lo, width) in enumerate(chunks):
        loads.append(
            pltpu.make_async_copy(ctrl_hbm.at[:, lo : lo + width], own[c], load_sem.at[1 + c])
        )
    loads.append(pltpu.make_async_copy(cwt_hbm, cwt_ref, load_sem.at[1 + n_chunks]))
    for item in loads:
        item.start()
    ty, tx = lax.axis_index("ty"), lax.axis_index("tx")
    rows = out_ref.shape[0]
    n_own = own[0].shape[0]
    n_slot = recv[0][0].shape[0]
    slot = n_slot // 8
    extent = n_own + n_slot

    def there(off):
        return jnp.logical_and(ty + off >= 0, ty + off < n_ty)

    def peer(row_off, col_off):
        return ty + row_off, lax.rem(tx + col_off + n_tx, n_tx)

    barrier = pltpu.get_barrier_semaphore()
    for row_off, col_off in DIRECTIONS:
        @pl.when(there(row_off))
        def _():
            pl.semaphore_signal(
                barrier, inc=1, device_id=peer(row_off, col_off), device_id_type=MESH
            )

    def copy(e, c, d):
        sign = -1 if e < 2 else 1
        row_off, col_off = DIRECTIONS[d]
        piece = pl.ds(d * slot, slot)
        return pltpu.make_async_remote_copy(
            src_ref=send[e][c].at[piece],
            dst_ref=recv[e][c].at[piece],
            send_sem=send_sem.at[e, c, d],
            recv_sem=recv_sem.at[e, c, d],
            device_id=peer(sign * row_off, sign * col_off),
            device_id_type=MESH,
        )

    def each(e, c, sending, action):
        sign = -1 if e < 2 else 1
        for d in ORDER:
            row_off = DIRECTIONS[d][0] * (sign if sending else -sign)
            if row_off == 0:
                action(copy(e, c, d))
            else:
                pl.when(there(row_off))(functools.partial(lambda e, c, d: action(copy(e, c, d)), e, c, d))

    def start(e, c):
        each(e, c, True, lambda item: item.start())

    def arrived(e, c):
        each(e, c, False, lambda item: item.wait_recv())

    def spread(wt_ref, cols_ref, mat, mat_t, base=0, count=extent):
        blocks, height, width = wt_ref.shape
        for b in range(blocks):
            index = cols_ref[b : b + 1, :]
            place_of = lax.broadcasted_iota(jnp.int32, (count, width), 0) + base
            hot = (place_of == index).astype(F32).astype(BF16)
            hi, lo = halves(wt_ref[b])
            span = pl.ds(b * height, height)
            if mat is not None:
                mat[0, span], mat[1, span] = halves(dot_nt(hi, hot) + dot_nt(lo, hot))
            if mat_t is not None:
                part = pl.ds(base, count)
                mat_t[0, part, span], mat_t[1, part, span] = halves(dot_nt(hot, hi) + dot_nt(hot, lo))

    def product(mat, row0, count, col0, depth, c, base):
        a_hi = mat[0, row0 : row0 + count, col0 : col0 + depth]
        a_lo = mat[1, row0 : row0 + count, col0 : col0 + depth]
        b_hi, b_lo = rhs[c][0, base : base + depth], rhs[c][1, base : base + depth]
        return dot(a_hi, b_hi) + (dot(a_hi, b_lo) + dot(a_lo, b_hi))

    def gathered(e, c):
        hi, lo = halves(recv[e][c][...])
        return dot(pick_t[...], hi) + dot(pick_t[...], lo)

    def place(c, base, value):
        rhs[c][0, base : base + value.shape[0]], rhs[c][1, base : base + value.shape[0]] = halves(value)

    def picked(c):
        return dot(pick[...], rhs[c][0, :n_own]) + dot(pick[...], rhs[c][1, :n_own])

    for e in range(4):
        sign = -1 if e < 2 else 1
        for d, (row_off, _) in enumerate(DIRECTIONS):
            if row_off:
                @pl.when(jnp.logical_not(there(-sign * row_off)))
                def _():
                    for c in range(n_chunks):
                        piece = recv[e][c].at[pl.ds(d * slot, slot)]
                        piece[...] = jnp.zeros(piece.shape, F32)

    loads[0].wait()
    spread(iwt_ref, icols_ref, None, imat_t, n_own, n_slot)
    limit = valid_ref[0, 0]
    edge = jnp.int32(2)
    edge += jnp.where(there(-1), 3, 0) + jnp.where(there(1), 3, 0)
    pl.semaphore_wait(barrier, edge)

    def keep(width):
        return lax.broadcasted_iota(jnp.int32, (rows, width), 0) < limit

    for c, (lo, width) in enumerate(chunks):
        loads[1 + c].wait()
        place(c, 0, jnp.where(keep(width), own[c][...], 0.0))
        send[0][c][...] = product(imat_t, n_own, n_slot, 0, rows, c, 0)
        start(0, c)
    spread(iwt_ref, icols_ref, None, imat_t, 0, n_own)
    for c in range(n_chunks):
        own[c][...] = product(imat_t, 0, n_own, 0, rows, c, 0)
    halo = jnp.concatenate([halo_ref[d : d + 1, :] for d in range(8)], axis=1)
    hot = (lax.broadcasted_iota(jnp.int32, (n_own, n_slot), 0) == halo).astype(F32)
    loads[-1].wait()
    pick_t[...] = hot.astype(BF16)
    pick[...] = hot.T.astype(BF16)
    spread(cwt_ref, ccols_ref, None, cmat_t)
    for c in range(n_chunks):
        arrived(0, c)
        place(c, 0, own[c][...] + gathered(0, c))
        send[1][c][...] = product(cmat_t, n_own, n_slot, 0, n_own, c, 0)
        start(1, c)
        own[c][...] = product(cmat_t, 0, n_own, 0, n_own, c, 0)
    spread(cwt_ref, ccols_ref, cmat, None)
    spread(iwt_ref, icols_ref, imat, None)
    for c in range(n_chunks):
        arrived(1, c)
        place(c, 0, own[c][...] + gathered(1, c))
        send[2][c][...] = picked(c)
        start(2, c)
        own[c][...] = product(cmat, 0, n_own, 0, n_own, c, 0)
    for c in range(n_chunks):
        arrived(2, c)
        place(c, n_own, recv[2][c][...])
        place(c, 0, own[c][...] + product(cmat, 0, n_own, n_own, n_slot, c, n_own))
        send[3][c][...] = picked(c)
        start(3, c)
        own[c][...] = product(imat, 0, rows, 0, n_own, c, 0)
    stores = []
    for c, (lo, width) in enumerate(chunks):
        arrived(3, c)
        place(c, n_own, recv[3][c][...])
        total = own[c][...] + product(imat, 0, rows, n_own, n_slot, c, n_own)
        own[c][...] = jnp.where(keep(width), total, 0.0)
        stores.append(
            pltpu.make_async_copy(own[c], out_ref.at[:, lo : lo + width], store_sem.at[c])
        )
        stores[c].start()
    for e in range(4):
        for c in range(n_chunks):
            each(e, c, True, lambda item: item.wait_send())
    for item in stores:
        item.wait()

OWN_ORDER = (0, 2, 3, 4, 5, 7, 1, 6)
FAR_ORDER = (0, 2, 3, 4, 5, 7, 6, 1)


def stacked(x):
    hi, lo = halves(x)
    return hi, jnp.concatenate([hi, lo], axis=0)


def folded(x):
    half = x.shape[0] // 2
    return x[:half] + x[half:]


def pair_kernel(
    n_ty, cuts, valid_ref, ctrl_hbm, iwt_hbm, icols_hbm, cwt_hbm, ccols_hbm, halo_hbm,
    out_ref, icols_ref, ccols_ref, halo_ref, ctrl, iwt, cwt, cwt_f, ccols_f, halo_f, xt, imat, imat_t, cmat, cmat_t, pick, pick_t,
    zp, s1, near, zf, r1o, bown, s2, r2, loc2, s3, r3, loc3, vacc,
    s4o, r4o, r4x, v_r, s6, r6, loc6, s5, r5, out_t, send_sem, recv_sem, load_sem,
):
    rows, feat = ctrl.shape
    half = feat // 2
    n_own, n_slot = pick.shape[1:]
    slot, group = n_slot // 8, n_slot // 4
    extent = n_own + n_slot
    n_x = 3 * group
    blocks = cwt.shape[0]
    ty, tx = lax.axis_index("ty"), lax.axis_index("tx")
    far = 1 - tx

    loads = [
        pltpu.make_async_copy(cwt_hbm, cwt, load_sem.at[0]),
        pltpu.make_async_copy(iwt_hbm, iwt, load_sem.at[1]),
        pltpu.make_async_copy(ctrl_hbm, ctrl, load_sem.at[2]),
        pltpu.make_async_copy(icols_hbm, icols_ref, load_sem.at[3]),
        pltpu.make_async_copy(ccols_hbm, ccols_ref, load_sem.at[4]),
        pltpu.make_async_copy(halo_hbm, halo_ref, load_sem.at[5]),
    ]
    for item in loads:
        item.start()

    def there(off):
        return jnp.logical_and(ty + off >= 0, ty + off < n_ty)

    barrier = pltpu.get_barrier_semaphore()
    partners = [(0, 1), (-1, 0), (1, 0)]
    for row_off, flip in partners:
        def greet(row_off=row_off, flip=flip):
            pl.semaphore_signal(
                barrier, inc=1, device_id=(ty + row_off, far if flip else tx), device_id_type=MESH
            )
        if row_off:
            pl.when(there(row_off))(greet)
        else:
            greet()

    arrivals, tags = [], {}
    both_there = jnp.logical_and(there(-1), there(1))
    one_there = jnp.logical_xor(there(-1), there(1))

    class Flow:
        def __init__(self, src, dst, tag=None):
            self.tag = tag or len(arrivals)
            self.keys = tags.setdefault(self.tag, [len(tags), None])[0], len(arrivals)
            arrivals.append(self)
            self.prepare(src, dst)

        def prepare(self, src, dst):
            self.copy = self.remote(src, dst, ty, far)

        def remote(self, src, dst, to_ty, to_tx):
            return pltpu.make_async_remote_copy(
                src_ref=src, dst_ref=dst, send_sem=send_sem.at[self.keys[0]], recv_sem=recv_sem.at[self.keys[1]],
                device_id=(to_ty, to_tx), device_id_type=MESH,
            )

        def start(self):
            before = tags[self.tag][1]
            if before is not None:
                before.sent()
            tags[self.tag][1] = self
            self.begin()

        def begin(self):
            self.copy.start()

        def arrived(self):
            self.copy.wait_recv()

        def sent(self):
            self.copy.wait_send()

    class Pair(Flow):
        def __init__(self, src, dst, sign, tag=None):
            self.sign = sign
            super().__init__(src, dst, tag)

        def prepare(self, src, dst):
            self.both = self.remote(src, dst, ty, far)
            self.parts = [
                self.remote(src.at[k], dst.at[k], ty + step, tx) for k, step in enumerate((self.sign, -self.sign))
            ]

        def begin(self):
            for part, step in zip(self.parts, (self.sign, -self.sign)):
                pl.when(there(step))(part.start)

        def arrived(self):
            pl.when(both_there)(self.both.wait_recv)
            pl.when(one_there)(self.parts[0].wait_recv)

        def sent(self):
            pl.when(both_there)(self.both.wait_send)
            pl.when(one_there)(self.parts[0].wait_send)

    def settle(keep=()):
        for entry in tags.values():
            if entry[1] is not None and entry[1] not in keep:
                entry[1].sent()
                entry[1] = None

    def go(*items):
        for item in items:
            item.start()
        return list(items)

    def wait(items):
        for item in items:
            item.arrived()

    def lane(count, width=group):
        return lax.broadcasted_iota(jnp.int32, (count, width), 1)

    def blend(first, second):
        return jnp.where(lane(first.shape[0]) < slot, first, second)

    def packed(x):
        top, low = x[: x.shape[0] // 2], x[x.shape[0] // 2 :]
        low = pltpu.roll(low, slot, 1)
        return blend(top, low), blend(low, top)

    def unpacked(first, second):
        low = pltpu.roll(blend(second, first), slot, 1)
        return jnp.concatenate([blend(first, second), low], axis=0)

    def dense(mat, mat_t, b, weights, index, order):
        where = index
        for place, d in enumerate(order):
            low = n_own + d * slot
            inside = jnp.logical_and(index >= low, index < low + slot)
            where = jnp.where(inside, index + (place - d) * slot, where)
        height, width = weights.shape
        hot = lax.broadcasted_iota(jnp.int32, (extent, width), 0) == where
        _, both = stacked(weights)
        span = pl.ds(b * height, height)
        hot = hot.astype(F32).astype(BF16)
        mat[0, span], mat[1, span] = halves(folded(dot_nt(both, hot)))
        turned = dot_nt(hot, both)
        mat_t[0, :, span], mat_t[1, :, span] = halves(turned[:, :height] + turned[:, height:])

    def choose(t, ref, order):
        halo = jnp.concatenate([ref[d : d + 1, :] for d in order], axis=1)
        hot = lax.broadcasted_iota(jnp.int32, (n_own, n_slot), 0) == halo
        hot = hot.astype(F32)
        pick[t], pick_t[t] = hot.astype(BF16), hot.T.astype(BF16)

    def scatter(t, pieces, lo=0):
        value = jnp.concatenate(pieces, axis=1) if len(pieces) > 1 else pieces[0]
        return folded(dot(stacked(value)[1], pick_t[t, lo : lo + value.shape[1]]))

    def apply(x, mat, lo, count):
        hi, both = x
        return folded(dot(both, mat[0, :, lo : lo + count])) + dot(hi, mat[1, :, lo : lo + count])

    def apply_t(x, mat, lo, count):
        hi, both = x
        return folded(dot(both, mat[0, lo : lo + count])) + dot(hi, mat[1, lo : lo + count])

    def gather(t, both, lo, count):
        return folded(dot(both, pick[t, :, lo : lo + count]))

    def within(side, lo, count):
        start = side * lo + (1 - side) * (half - lo - count)
        return pl.ds(pl.multiple_of(start, 16), count)

    def placed(side, lo, count):
        start = side * (half + lo) + (1 - side) * (half - lo - count)
        return pl.ds(pl.multiple_of(start, 16), count)

    def mine(lo, count):
        return placed(tx, lo, count)

    def theirs(lo, count):
        return placed(far, lo, count)

    def blank(ref):
        ref[...] = jnp.zeros(ref.shape, ref.dtype)

    @pl.when(jnp.logical_not(there(-1)))
    def _():
        for ref in (near.at[0], r2.at[0], r3.at[1], r4o.at[1], r6.at[1], r5.at[1]):
            blank(ref)

    @pl.when(jnp.logical_not(there(1)))
    def _():
        for ref in (near.at[1], r2.at[1], r3.at[0], r4o.at[0], r6.at[0], r5.at[0]):
            blank(ref)

    loads[0].wait()
    pl.semaphore_wait(barrier, 1 + jnp.where(there(-1), 1, 0) + jnp.where(there(1), 1, 0))
    for item in loads[3:]:
        item.wait()
    tables = go(Flow(ccols_ref, ccols_f), Flow(halo_ref, halo_f))
    weights = go(Flow(cwt, cwt_f))

    limit = valid_ref[0, 0]
    loads[1].wait()
    for b in range(iwt.shape[0]):
        dense(imat, imat_t, b, iwt[b], icols_ref[b : b + 1, :], OWN_ORDER)
    loads[2].wait()
    tile = 128
    for lo in range(0, feat, tile):
        live = lax.broadcasted_iota(jnp.int32, (rows, tile), 0) < limit
        piece = jnp.where(live, ctrl[:, lo : lo + tile], 0.0).T
        xt[0, lo : lo + tile], xt[1, lo : lo + tile] = halves(piece)
    last = []
    for q in range(2):
        span = slice(q * half, (q + 1) * half)
        both = jnp.concatenate([xt[0, span], xt[1, span]], axis=0)
        value = apply((xt[0, span], both), imat, n_own, n_slot)
        s1[0, q], near[2, q], s1[1, q] = (value[:, g * group : (g + 1) * group] for g in range(3))
        last.append(value[:, n_x:])
    s1[0, 2], s1[1, 2] = packed(jnp.concatenate(last, axis=0))
    first = go(Pair(s1, near.at[0:2], 1))
    for q in range(2):
        span = slice(q * half, (q + 1) * half)
        both = jnp.concatenate([xt[0, span], xt[1, span]], axis=0)
        zp[span] = apply((xt[0, span], both), imat, 0, n_own)
    choose(0, halo_ref, OWN_ORDER)
    wait(first)
    extra = unpacked(near[0, 2], near[1, 2])
    for q in range(2):
        span = slice(q * half, (q + 1) * half)
        zp[span] = zp[span] + scatter(0, [extra[span]], n_x)
    crossed = []
    for lo, count in cuts:
        span = pl.ds(lo, count)
        crossed.append(go(
            Flow(zp.at[theirs(lo, count)], zf.at[span]),
            Flow(near.at[:, far, within(far, lo, count)], r1o.at[:, span]),
        ))
    for b in range(blocks):
        dense(cmat.at[0], cmat_t.at[0], b, cwt[b], ccols_ref[b : b + 1, :], OWN_ORDER)
    wait(tables)
    choose(1, halo_f, FAR_ORDER)
    wait(weights)
    for b in range(blocks):
        dense(cmat.at[1], cmat_t.at[1], b, cwt_f[b], ccols_f[b : b + 1, :], FAR_ORDER)

    second, third, fourth, fifth, sixth, sides, whole = {}, {}, {}, {}, {}, {}, {}
    n = len(cuts)

    def swap(c, sent, got, kept, sign, tag, value):
        span = pl.ds(*cuts[c])
        last = []
        for t in range(2):
            sent[0, t, span], kept[t, span] = value[t][:, :group], value[t][:, group : 2 * group]
            sent[1, t, span] = value[t][:, 2 * group : n_x]
            last.append(value[t][:, n_x:])
        sent[0, 2, span], sent[1, 2, span] = blend(last[0], last[1]), blend(last[1], last[0])
        return go(Pair(sent.at[:, :, span], got.at[:, :, span], sign, tag))

    def swapped(c, got, kept):
        span = pl.ds(*cuts[c])
        return [
            jnp.concatenate([
                got[0, 1 - t, span], kept[1 - t, span], got[1, 1 - t, span],
                blend(got[t, 2, span], got[1 - t, 2, span]),
            ], axis=1)
            for t in range(2)
        ]

    def adjoint(c):
        lo, count = cuts[c]
        span = pl.ds(lo, count)
        here = within(tx, lo, count)
        wait(crossed[c])
        z = [
            zp[mine(lo, count)] + scatter(0, [r1o[g, span] for g in (0, 2, 1)]),
            zf[span] + scatter(1, [near[g, tx, here] for g in (0, 2, 1)]),
        ]
        z = [stacked(item) for item in z]
        second[c] = swap(c, s2, r2, loc2, 1, "b", [apply(z[t], cmat.at[t], n_own, n_slot) for t in range(2)])
        for t in range(2):
            bown[t, span] = apply(z[t], cmat.at[t], 0, n_own)

    def middle(c):
        span = pl.ds(*cuts[c])
        wait(second[c])
        slots = swapped(c, r2, loc2)
        w = [stacked(bown[t, span] + scatter(t, [slots[t]])) for t in range(2)]
        third[c] = swap(c, s3, r3, loc3, -1, "w", [gather(t, w[t][1], 0, n_slot) for t in range(2)])
        for t in range(2):
            vacc[t, span] = apply_t(w[t], cmat_t.at[t], 0, n_own)

    def forward(c):
        lo, count = cuts[c]
        span, part = pl.ds(lo, count), pl.ds(lo // 2, count // 2)
        wait(third[c])
        slots = swapped(c, r3, loc3)
        v = [None, None]
        for t in (1, 0):
            v[t] = vacc[t, span] + apply_t(stacked(slots[t]), cmat_t.at[t], n_own, n_slot)
            vacc[t, span] = v[t]
            if t:
                whole[c] = go(Flow(vacc.at[1, span], v_r.at[span]))
        value = gather(0, stacked(v[0])[1], 0, n_slot)
        s4o[0, span], r4o[2, span], s4o[1, span] = (value[:, g * group : (g + 1) * group] for g in range(3))
        sides[c] = go(Pair(s4o.at[:, span], r4o.at[0:2, span], -1, "s"))
        s6[0, 2, part], s6[1, 2, part] = packed(value[:, n_x:])
        value = gather(1, stacked(v[1])[1], 0, n_x)
        loc6[span] = value[:, group : 2 * group]
        for q in range(2):
            rows_q = slice(q * (count // 2), (q + 1) * (count // 2))
            s6[0, q, part], s6[1, q, part] = value[rows_q, :group], value[rows_q, 2 * group :]

    def leave(c):
        span = pl.ds(*cuts[c])
        wait(sides[c])
        sixth[c] = go(Flow(r4o.at[:, span], r4x.at[:, span]))

    def joined(c, count):
        lo = cuts[c][0]
        end = sum(cuts[c + count - 1])
        return pl.ds(lo // 2, (end - lo) // 2)

    def spare(c, count):
        part = joined(c, count)
        fourth[c] = go(Pair(s6.at[:, :, part], r6.at[:, :, part], -1))

    def relay(c, count=1):
        for k in range(c, c + count):
            wait(whole[k])
            lo, width = cuts[k]
            part = pl.ds(lo // 2, width // 2)
            s5[0, part], s5[1, part] = packed(gather(0, stacked(v_r[pl.ds(lo, width)])[1], n_x, group))
        part = joined(c, count)
        fifth[c] = go(Pair(s5.at[:, part], r5.at[:, part], -1))

    def finish(q, c, stages=(0, 1)):
        lo, count = cuts[c]
        span, part = pl.ds(lo, count), pl.ds(lo // 2, count // 2)
        place = theirs(lo, count) if q else mine(lo, count)
        if 0 in stages:
            wait(fifth.get(c, ()) if q else fourth.get(c, ()))
            last = unpacked(r5[0, part], r5[1, part]) if q else unpacked(r6[0, 2, part], r6[1, 2, part])
            main = v_r[span] if q else vacc[0, span]
        if 1 in stages and q:
            wait(sixth[c])
            outer = [r4x[g, span] for g in (0, 2, 1)]
        elif 1 in stages:
            outer = [jnp.concatenate([r6[k, 0, part], r6[k, 1, part]], axis=0) for k in range(2)]
            outer.insert(1, loc6[span])
        if len(stages) == 2:
            both = stacked(jnp.concatenate([main, *outer, last], axis=1))
            out_t[place] = apply_t(both, imat_t, 0, extent)
        elif 0 in stages:
            out_t[place] = apply_t(stacked(main), imat_t, 0, n_own) + apply_t(stacked(last), imat_t, n_own + n_x, group)
        else:
            both = stacked(jnp.concatenate(outer, axis=1))
            out_t[place] = out_t[place] + apply_t(both, imat_t, n_own, n_x)

    def ready(r):
        return max([c for c in range(n) if half + cuts[c][0] < (r + 1) * tile], default=-1)

    def store(c):
        for r in range(feat // tile):
            if ready(r) == c:
                block = far * r + tx * (feat // tile - 1 - r)
                span = pl.ds(pl.multiple_of(block * tile, tile), tile)
                live = lax.broadcasted_iota(jnp.int32, (rows, tile), 0) < limit
                out_ref[:, span] = jnp.where(live, out_t[span].T, 0.0)

    for step in range(n + 3):
        order = ((adjoint, 0), (middle, 1), (leave, 3), (forward, 2))
        if step > n:
            order = ((forward, 2), (leave, 3))
        for stage, lag in order:
            if 0 <= step - lag < n:
                stage(step - lag)
        if step == n:
            spare(0, n - 2)
        if step == n + 1:
            relay(0, n - 2)
            spare(n - 2, 2)
            for c in range(n - 2):
                finish(0, c)
    relay(n - 2)
    finish(0, n - 2)
    relay(n - 1)
    for c in range(n - 2):
        finish(1, c)
    finish(0, n - 1)
    for c in range(-1, n - 2):
        store(c)
    finish(1, n - 2)
    store(n - 2)
    settle(sixth[n - 1] + fifth[n - 1])
    finish(1, n - 1, (0,))
    finish(1, n - 1, (1,))
    store(n - 1)
    settle()


def split(total, parts):
    unit = total // 16
    sizes = [16 * (unit // parts + (1 if k < unit % parts else 0)) for k in range(parts)]
    starts = [sum(sizes[:k]) for k in range(parts)]
    return tuple(zip(starts, sizes))


def pair_call(n_ty, ctrl, interp_wt, interp_cols, conv_wt, conv_cols, halo_index, valid):
    rows, feat = ctrl.shape[2:]
    n_own = conv_wt.shape[2] * conv_wt.shape[3]
    n_slot = halo_index.shape[2] * halo_index.shape[3]
    extent, group, half = n_own + n_slot, n_slot // 4, feat // 2
    cuts = split(half, 4)
    pin = functools.partial(pltpu.with_memory_space_constraint, memory_space=pltpu.HBM)
    hbm = pl.BlockSpec(memory_space=pltpu.HBM)
    vmem = pl.BlockSpec(memory_space=pltpu.VMEM)

    def f32(*shape):
        return pltpu.VMEM(shape, F32)

    def bf16(*shape):
        return pltpu.VMEM(shape, BF16)

    scratch = [
        *[pltpu.VMEM(item.shape[2:], jnp.int32) for item in (interp_cols, conv_cols, halo_index)],
        f32(rows, feat), f32(*interp_wt.shape[2:]), f32(*conv_wt.shape[2:]), f32(*conv_wt.shape[2:]),
        pltpu.VMEM(conv_cols.shape[2:], jnp.int32), pltpu.VMEM(halo_index.shape[2:], jnp.int32),
        bf16(2, feat, rows), bf16(2, rows, extent), bf16(2, extent, rows),
        bf16(2, 2, n_own, extent), bf16(2, 2, extent, n_own), bf16(2, n_own, n_slot), bf16(2, n_slot, n_own),
        f32(feat, n_own), f32(2, 3, half, group), f32(3, 3, half, group),
        f32(half, n_own), f32(3, half, group), f32(2, half, n_own),
        f32(2, 3, half, group), f32(2, 3, half, group), f32(2, half, group),
        f32(2, 3, half, group), f32(2, 3, half, group), f32(2, half, group), f32(2, half, n_own),
        f32(2, half, group), f32(3, half, group), f32(3, half, group), f32(half, n_own),
        f32(2, 3, half // 2, group), f32(2, 3, half // 2, group), f32(half, group),
        f32(2, half // 2, group), f32(2, half // 2, group),
        f32(feat, rows),
    ]
    dma = pltpu.SemaphoreType.DMA
    scratch += [dma((8 + 5 * len(cuts) + 1,)), dma((5 + 8 * len(cuts),)), dma((6,))]
    return pl.pallas_call(
        functools.partial(pair_kernel, n_ty, cuts),
        out_shape=jax.ShapeDtypeStruct((rows, feat), F32),
        in_specs=[pl.BlockSpec(memory_space=pltpu.SMEM)] + [hbm] * 6,
        out_specs=vmem,
        scratch_shapes=scratch,
        compiler_params=pltpu.CompilerParams(
            collective_id=0, has_side_effects=True, vmem_limit_bytes=52 * 1024 * 1024
        ),
    )(
        valid, pin(ctrl[0, 0]), pin(interp_wt[0, 0]), pin(interp_cols[0, 0]), pin(conv_wt[0, 0]),
        pin(conv_cols[0, 0]), pin(halo_index[0, 0]),
    )


def pairs_fit(n_tx, ctrl, halo_index):
    slot = halo_index.shape[3]
    return n_tx == 2 and halo_index.shape[2] == 8 and slot == 64 and ctrl.shape[3] % 128 == 0


def solution(mesh):
    n_ty, n_tx = mesh.shape["ty"], mesh.shape["tx"]

    def body(ctrl, interp_wt, interp_cols, conv_wt, conv_cols, halo_index, valid):
        rows, feat = ctrl.shape[2:]
        n_own = conv_wt.shape[2] * conv_wt.shape[3]
        n_slot = halo_index.shape[2] * halo_index.shape[3]
        extent = n_own + n_slot
        if pairs_fit(n_tx, ctrl, halo_index) and rows == n_own:
            args = ctrl, interp_wt, interp_cols, conv_wt, conv_cols, halo_index, valid
            return pair_call(n_ty, *args)[None, None]
        tiles = feat // 128
        first = 128 * max(tiles - tiles // 2, 1)
        chunks = ((0, first), (first, feat - first)) if feat > first else ((0, feat),)
        widths = [width for _, width in chunks]
        pin = functools.partial(pltpu.with_memory_space_constraint, memory_space=pltpu.HBM)
        hbm = pl.BlockSpec(memory_space=pltpu.HBM)
        vmem = pl.BlockSpec(memory_space=pltpu.VMEM)
        scratch = [
            pltpu.VMEM(interp_wt.shape[2:], F32),
            pltpu.VMEM(conv_wt.shape[2:], F32),
            pltpu.VMEM((2, rows, extent), BF16),
            pltpu.VMEM((2, extent, rows), BF16),
            pltpu.VMEM((2, n_own, extent), BF16),
            pltpu.VMEM((2, extent, n_own), BF16),
            pltpu.VMEM((n_slot, n_own), BF16),
            pltpu.VMEM((n_own, n_slot), BF16),
        ]
        assert rows == n_own
        scratch += [pltpu.VMEM((n_own, width), F32) for width in widths]
        scratch += [pltpu.VMEM((2, extent, width), BF16) for width in widths]
        scratch += [pltpu.VMEM((n_slot, width), F32) for _ in range(8) for width in widths]
        scratch += [pltpu.SemaphoreType.DMA((4, len(chunks), 8))] * 2
        scratch += [pltpu.SemaphoreType.DMA((2 + len(chunks),)), pltpu.SemaphoreType.DMA((len(chunks),))]
        out = pl.pallas_call(
            functools.partial(kernel, n_ty, n_tx, chunks),
            out_shape=jax.ShapeDtypeStruct((rows, feat), F32),
            in_specs=[pl.BlockSpec(memory_space=pltpu.SMEM), hbm, hbm, vmem, hbm, vmem, vmem],
            out_specs=pl.BlockSpec(memory_space=pl.ANY),
            scratch_shapes=scratch,
            compiler_params=pltpu.CompilerParams(
                collective_id=0, has_side_effects=True, vmem_limit_bytes=44 * 1024 * 1024
            ),
        )(
            valid, pin(ctrl[0, 0]), pin(interp_wt[0, 0]), pin(interp_cols[0, 0]), pin(conv_wt[0, 0]),
            pin(conv_cols[0, 0]), pin(halo_index[0, 0]),
        )
        return out[None, None]

    placed = (
        P("ty", "tx", None, None),
        P("ty", "tx", None, None, None),
        P("ty", "tx", None, None),
        P("ty", "tx", None, None, None),
        P("ty", "tx", None, None),
        P("ty", "tx", None, None),
        P("ty", "tx"),
    )
    return jax.shard_map(
        body, mesh=mesh, in_specs=placed, out_specs=P("ty", "tx", None, None), check_vma=False
    )
```

```python
import functools

import jax
import jax.numpy as jnp
from jax import lax
from jax.experimental import pallas as pl
from jax.experimental.pallas import tpu as pltpu
from jax.sharding import PartitionSpec as P

MESH = pl.DeviceIdType.MESH
DIRECTIONS = ((-1, -1), (-1, 0), (-1, 1), (0, -1), (0, 1), (1, -1), (1, 0), (1, 1))
ORDER = (0, 2, 5, 7, 3, 4, 1, 6)
F32, BF16 = jnp.float32, jnp.bfloat16


def halves(x):
    hi = x.astype(BF16)
    return hi, (x - hi.astype(F32)).astype(BF16)


def dot(a, b):
    return jnp.dot(a, b, preferred_element_type=F32)


def dot_nt(a, b):
    return lax.dot_general(a, b, (((1,), (1,)), ((), ())), preferred_element_type=F32)


def kernel(
    n_ty, n_tx, chunks, valid_ref, ctrl_hbm, iwt_hbm, icols_ref, cwt_hbm, ccols_ref, halo_ref,
    out_ref, iwt_ref, cwt_ref, imat, imat_t, cmat, cmat_t, pick, pick_t, *rest,
):
    n_chunks = len(chunks)
    send_sem, recv_sem, load_sem, store_sem = rest[-4:]
    buffers = rest[:-4]
    own = buffers[:n_chunks]
    rhs = buffers[n_chunks : 2 * n_chunks]
    send = [buffers[(2 + e) * n_chunks : (3 + e) * n_chunks] for e in range(4)]
    recv = [buffers[(6 + e) * n_chunks : (7 + e) * n_chunks] for e in range(4)]
    loads = [pltpu.make_async_copy(iwt_hbm, iwt_ref, load_sem.at[0])]
    for c, (lo, width) in enumerate(chunks):
        loads.append(
            pltpu.make_async_copy(ctrl_hbm.at[:, lo : lo + width], own[c], load_sem.at[1 + c])
        )
    loads.append(pltpu.make_async_copy(cwt_hbm, cwt_ref, load_sem.at[1 + n_chunks]))
    for item in loads:
        item.start()
    ty, tx = lax.axis_index("ty"), lax.axis_index("tx")
    rows = out_ref.shape[0]
    n_own = own[0].shape[0]
    n_slot = recv[0][0].shape[0]
    slot = n_slot // 8
    extent = n_own + n_slot

    def there(off):
        return jnp.logical_and(ty + off >= 0, ty + off < n_ty)

    def peer(row_off, col_off):
        return ty + row_off, lax.rem(tx + col_off + n_tx, n_tx)

    barrier = pltpu.get_barrier_semaphore()
    for row_off, col_off in DIRECTIONS:
        @pl.when(there(row_off))
        def _():
            pl.semaphore_signal(
                barrier, inc=1, device_id=peer(row_off, col_off), device_id_type=MESH
            )

    def copy(e, c, d):
        sign = -1 if e < 2 else 1
        row_off, col_off = DIRECTIONS[d]
        piece = pl.ds(d * slot, slot)
        return pltpu.make_async_remote_copy(
            src_ref=send[e][c].at[piece],
            dst_ref=recv[e][c].at[piece],
            send_sem=send_sem.at[e, c, d],
            recv_sem=recv_sem.at[e, c, d],
            device_id=peer(sign * row_off, sign * col_off),
            device_id_type=MESH,
        )

    def each(e, c, sending, action):
        sign = -1 if e < 2 else 1
        for d in ORDER:
            row_off = DIRECTIONS[d][0] * (sign if sending else -sign)
            if row_off == 0:
                action(copy(e, c, d))
            else:
                pl.when(there(row_off))(functools.partial(lambda e, c, d: action(copy(e, c, d)), e, c, d))

    def start(e, c):
        each(e, c, True, lambda item: item.start())

    def arrived(e, c):
        each(e, c, False, lambda item: item.wait_recv())

    def spread(wt_ref, cols_ref, mat, mat_t, base=0, count=extent):
        blocks, height, width = wt_ref.shape
        for b in range(blocks):
            index = cols_ref[b : b + 1, :]
            place_of = lax.broadcasted_iota(jnp.int32, (count, width), 0) + base
            hot = (place_of == index).astype(F32).astype(BF16)
            hi, lo = halves(wt_ref[b])
            span = pl.ds(b * height, height)
            if mat is not None:
                mat[0, span], mat[1, span] = halves(dot_nt(hi, hot) + dot_nt(lo, hot))
            if mat_t is not None:
                part = pl.ds(base, count)
                mat_t[0, part, span], mat_t[1, part, span] = halves(dot_nt(hot, hi) + dot_nt(hot, lo))

    def product(mat, row0, count, col0, depth, c, base):
        a_hi = mat[0, row0 : row0 + count, col0 : col0 + depth]
        a_lo = mat[1, row0 : row0 + count, col0 : col0 + depth]
        b_hi, b_lo = rhs[c][0, base : base + depth], rhs[c][1, base : base + depth]
        return dot(a_hi, b_hi) + (dot(a_hi, b_lo) + dot(a_lo, b_hi))

    def gathered(e, c):
        hi, lo = halves(recv[e][c][...])
        return dot(pick_t[...], hi) + dot(pick_t[...], lo)

    def place(c, base, value):
        rhs[c][0, base : base + value.shape[0]], rhs[c][1, base : base + value.shape[0]] = halves(value)

    def picked(c):
        return dot(pick[...], rhs[c][0, :n_own]) + dot(pick[...], rhs[c][1, :n_own])

    for e in range(4):
        sign = -1 if e < 2 else 1
        for d, (row_off, _) in enumerate(DIRECTIONS):
            if row_off:
                @pl.when(jnp.logical_not(there(-sign * row_off)))
                def _():
                    for c in range(n_chunks):
                        piece = recv[e][c].at[pl.ds(d * slot, slot)]
                        piece[...] = jnp.zeros(piece.shape, F32)

    loads[0].wait()
    spread(iwt_ref, icols_ref, None, imat_t, n_own, n_slot)
    limit = valid_ref[0, 0]
    edge = jnp.int32(2)
    edge += jnp.where(there(-1), 3, 0) + jnp.where(there(1), 3, 0)
    pl.semaphore_wait(barrier, edge)

    def keep(width):
        return lax.broadcasted_iota(jnp.int32, (rows, width), 0) < limit

    for c, (lo, width) in enumerate(chunks):
        loads[1 + c].wait()
        place(c, 0, jnp.where(keep(width), own[c][...], 0.0))
        send[0][c][...] = product(imat_t, n_own, n_slot, 0, rows, c, 0)
        start(0, c)
    spread(iwt_ref, icols_ref, None, imat_t, 0, n_own)
    for c in range(n_chunks):
        own[c][...] = product(imat_t, 0, n_own, 0, rows, c, 0)
    halo = jnp.concatenate([halo_ref[d : d + 1, :] for d in range(8)], axis=1)
    hot = (lax.broadcasted_iota(jnp.int32, (n_own, n_slot), 0) == halo).astype(F32)
    loads[-1].wait()
    pick_t[...] = hot.astype(BF16)
    pick[...] = hot.T.astype(BF16)
    spread(cwt_ref, ccols_ref, None, cmat_t)
    for c in range(n_chunks):
        arrived(0, c)
        place(c, 0, own[c][...] + gathered(0, c))
        send[1][c][...] = product(cmat_t, n_own, n_slot, 0, n_own, c, 0)
        start(1, c)
        own[c][...] = product(cmat_t, 0, n_own, 0, n_own, c, 0)
    spread(cwt_ref, ccols_ref, cmat, None)
    spread(iwt_ref, icols_ref, imat, None)
    for c in range(n_chunks):
        arrived(1, c)
        place(c, 0, own[c][...] + gathered(1, c))
        send[2][c][...] = picked(c)
        start(2, c)
        own[c][...] = product(cmat, 0, n_own, 0, n_own, c, 0)
    for c in range(n_chunks):
        arrived(2, c)
        place(c, n_own, recv[2][c][...])
        place(c, 0, own[c][...] + product(cmat, 0, n_own, n_own, n_slot, c, n_own))
        send[3][c][...] = picked(c)
        start(3, c)
        own[c][...] = product(imat, 0, rows, 0, n_own, c, 0)
    stores = []
    for c, (lo, width) in enumerate(chunks):
        arrived(3, c)
        place(c, n_own, recv[3][c][...])
        total = own[c][...] + product(imat, 0, rows, n_own, n_slot, c, n_own)
        own[c][...] = jnp.where(keep(width), total, 0.0)
        stores.append(
            pltpu.make_async_copy(own[c], out_ref.at[:, lo : lo + width], store_sem.at[c])
        )
        stores[c].start()
    for e in range(4):
        for c in range(n_chunks):
            each(e, c, True, lambda item: item.wait_send())
    for item in stores:
        item.wait()

OWN_ORDER = (0, 2, 3, 4, 5, 7, 1, 6)
FAR_ORDER = (0, 2, 3, 4, 5, 7, 6, 1)


def stacked(x):
    hi, lo = halves(x)
    return hi, jnp.concatenate([hi, lo], axis=0)


def folded(x):
    half = x.shape[0] // 2
    return x[:half] + x[half:]


def pair_kernel(
    n_ty, cuts, valid_ref, ctrl_hbm, iwt_hbm, icols_hbm, cwt_hbm, ccols_hbm, halo_hbm,
    out_ref, icols_ref, ccols_ref, halo_ref, ctrl, iwt, cwt, cwt_f, ccols_f, halo_f, xt, imat, imat_t, cmat, cmat_t, pick, pick_t,
    zp, s1, near, zf, r1o, bown, s2, r2, loc2, s3, r3, loc3, vacc,
    s4o, r4o, r4x, v_r, s6, r6, loc6, s5, r5, out_t, send_sem, recv_sem, load_sem,
):
    rows, feat = ctrl.shape
    half = feat // 2
    n_own, n_slot = pick.shape[1:]
    slot, group = n_slot // 8, n_slot // 4
    extent = n_own + n_slot
    n_x = 3 * group
    blocks = cwt.shape[0]
    ty, tx = lax.axis_index("ty"), lax.axis_index("tx")
    far = 1 - tx

    loads = [
        pltpu.make_async_copy(cwt_hbm, cwt, load_sem.at[0]),
        pltpu.make_async_copy(iwt_hbm, iwt, load_sem.at[1]),
        pltpu.make_async_copy(ctrl_hbm, ctrl, load_sem.at[2]),
        pltpu.make_async_copy(icols_hbm, icols_ref, load_sem.at[3]),
        pltpu.make_async_copy(ccols_hbm, ccols_ref, load_sem.at[4]),
        pltpu.make_async_copy(halo_hbm, halo_ref, load_sem.at[5]),
    ]
    for item in loads:
        item.start()

    def there(off):
        return jnp.logical_and(ty + off >= 0, ty + off < n_ty)

    barrier = pltpu.get_barrier_semaphore()
    partners = [(0, 1), (-1, 0), (1, 0)]
    for row_off, flip in partners:
        def greet(row_off=row_off, flip=flip):
            pl.semaphore_signal(
                barrier, inc=1, device_id=(ty + row_off, far if flip else tx), device_id_type=MESH
            )
        if row_off:
            pl.when(there(row_off))(greet)
        else:
            greet()

    arrivals, tags = [], {}
    both_there = jnp.logical_and(there(-1), there(1))
    one_there = jnp.logical_xor(there(-1), there(1))

    class Flow:
        def __init__(self, src, dst, tag=None):
            self.tag = tag or len(arrivals)
            self.keys = tags.setdefault(self.tag, [len(tags), None])[0], len(arrivals)
            arrivals.append(self)
            self.prepare(src, dst)

        def prepare(self, src, dst):
            self.copy = self.remote(src, dst, ty, far)

        def remote(self, src, dst, to_ty, to_tx):
            return pltpu.make_async_remote_copy(
                src_ref=src, dst_ref=dst, send_sem=send_sem.at[self.keys[0]], recv_sem=recv_sem.at[self.keys[1]],
                device_id=(to_ty, to_tx), device_id_type=MESH,
            )

        def start(self):
            before = tags[self.tag][1]
            if before is not None:
                before.sent()
            tags[self.tag][1] = self
            self.begin()

        def begin(self):
            self.copy.start()

        def arrived(self):
            self.copy.wait_recv()

        def sent(self):
            self.copy.wait_send()

    class Pair(Flow):
        def __init__(self, src, dst, sign, tag=None):
            self.sign = sign
            super().__init__(src, dst, tag)

        def prepare(self, src, dst):
            self.both = self.remote(src, dst, ty, far)
            self.parts = [
                self.remote(src.at[k], dst.at[k], ty + step, tx) for k, step in enumerate((self.sign, -self.sign))
            ]

        def begin(self):
            for part, step in zip(self.parts, (self.sign, -self.sign)):
                pl.when(there(step))(part.start)

        def arrived(self):
            pl.when(both_there)(self.both.wait_recv)
            pl.when(one_there)(self.parts[0].wait_recv)

        def sent(self):
            pl.when(both_there)(self.both.wait_send)
            pl.when(one_there)(self.parts[0].wait_send)

    def settle(keep=()):
        for entry in tags.values():
            if entry[1] is not None and entry[1] not in keep:
                entry[1].sent()
                entry[1] = None

    def go(*items):
        for item in items:
            item.start()
        return list(items)

    def wait(items):
        for item in items:
            item.arrived()

    def lane(count, width=group):
        return lax.broadcasted_iota(jnp.int32, (count, width), 1)

    def blend(first, second):
        return jnp.where(lane(first.shape[0]) < slot, first, second)

    def packed(x):
        top, low = x[: x.shape[0] // 2], x[x.shape[0] // 2 :]
        low = pltpu.roll(low, slot, 1)
        return blend(top, low), blend(low, top)

    def unpacked(first, second):
        low = pltpu.roll(blend(second, first), slot, 1)
        return jnp.concatenate([blend(first, second), low], axis=0)

    def dense(mat, mat_t, b, weights, index, order):
        where = index
        for place, d in enumerate(order):
            low = n_own + d * slot
            inside = jnp.logical_and(index >= low, index < low + slot)
            where = jnp.where(inside, index + (place - d) * slot, where)
        height, width = weights.shape
        hot = lax.broadcasted_iota(jnp.int32, (extent, width), 0) == where
        _, both = stacked(weights)
        span = pl.ds(b * height, height)
        hot = hot.astype(F32).astype(BF16)
        mat[0, span], mat[1, span] = halves(folded(dot_nt(both, hot)))
        turned = dot_nt(hot, both)
        mat_t[0, :, span], mat_t[1, :, span] = halves(turned[:, :height] + turned[:, height:])

    def choose(t, ref, order):
        halo = jnp.concatenate([ref[d : d + 1, :] for d in order], axis=1)
        hot = lax.broadcasted_iota(jnp.int32, (n_own, n_slot), 0) == halo
        hot = hot.astype(F32)
        pick[t], pick_t[t] = hot.astype(BF16), hot.T.astype(BF16)

    def scatter(t, pieces, lo=0):
        value = jnp.concatenate(pieces, axis=1) if len(pieces) > 1 else pieces[0]
        return folded(dot(stacked(value)[1], pick_t[t, lo : lo + value.shape[1]]))

    def apply(x, mat, lo, count):
        hi, both = x
        return folded(dot(both, mat[0, :, lo : lo + count])) + dot(hi, mat[1, :, lo : lo + count])

    def apply_t(x, mat, lo, count):
        hi, both = x
        return folded(dot(both, mat[0, lo : lo + count])) + dot(hi, mat[1, lo : lo + count])

    def gather(t, both, lo, count):
        return folded(dot(both, pick[t, :, lo : lo + count]))

    def within(side, lo, count):
        start = side * lo + (1 - side) * (half - lo - count)
        return pl.ds(pl.multiple_of(start, 16), count)

    def placed(side, lo, count):
        start = side * (half + lo) + (1 - side) * (half - lo - count)
        return pl.ds(pl.multiple_of(start, 16), count)

    def mine(lo, count):
        return placed(tx, lo, count)

    def theirs(lo, count):
        return placed(far, lo, count)

    def blank(ref):
        ref[...] = jnp.zeros(ref.shape, ref.dtype)

    @pl.when(jnp.logical_not(there(-1)))
    def _():
        for ref in (near.at[0], r2.at[0], r3.at[1], r4o.at[1], r6.at[1], r5.at[1]):
            blank(ref)

    @pl.when(jnp.logical_not(there(1)))
    def _():
        for ref in (near.at[1], r2.at[1], r3.at[0], r4o.at[0], r6.at[0], r5.at[0]):
            blank(ref)

    loads[0].wait()
    pl.semaphore_wait(barrier, 1 + jnp.where(there(-1), 1, 0) + jnp.where(there(1), 1, 0))
    for item in loads[3:]:
        item.wait()
    tables = go(Flow(ccols_ref, ccols_f, "t0"), Flow(halo_ref, halo_f, "t1"))
    weights = go(Flow(cwt, cwt_f, "x"))

    limit = valid_ref[0, 0]
    loads[1].wait()
    for b in range(iwt.shape[0]):
        dense(imat, imat_t, b, iwt[b], icols_ref[b : b + 1, :], OWN_ORDER)
    loads[2].wait()
    tile = 128
    for lo in range(0, feat, tile):
        live = lax.broadcasted_iota(jnp.int32, (rows, tile), 0) < limit
        piece = jnp.where(live, ctrl[:, lo : lo + tile], 0.0).T
        xt[0, lo : lo + tile], xt[1, lo : lo + tile] = halves(piece)
    last = []
    for q in range(2):
        span = slice(q * half, (q + 1) * half)
        both = jnp.concatenate([xt[0, span], xt[1, span]], axis=0)
        value = apply((xt[0, span], both), imat, n_own, n_slot)
        s1[0, q], near[2, q], s1[1, q] = (value[:, g * group : (g + 1) * group] for g in range(3))
        last.append(value[:, n_x:])
    s1[0, 2], s1[1, 2] = packed(jnp.concatenate(last, axis=0))
    first = go(Pair(s1, near.at[0:2], 1, "f"))
    for q in range(2):
        span = slice(q * half, (q + 1) * half)
        both = jnp.concatenate([xt[0, span], xt[1, span]], axis=0)
        zp[span] = apply((xt[0, span], both), imat, 0, n_own)
    choose(0, halo_ref, OWN_ORDER)
    wait(first)
    extra = unpacked(near[0, 2], near[1, 2])
    for q in range(2):
        span = slice(q * half, (q + 1) * half)
        zp[span] = zp[span] + scatter(0, [extra[span]], n_x)
    crossed = []
    for c, (lo, count) in enumerate(cuts):
        span = pl.ds(lo, count)
        crossed.append(go(
            Flow(zp.at[theirs(lo, count)], zf.at[span], ("z", c)),
            Flow(near.at[:, far, within(far, lo, count)], r1o.at[:, span], ("g", c)),
        ))
    for b in range(blocks):
        dense(cmat.at[0], cmat_t.at[0], b, cwt[b], ccols_ref[b : b + 1, :], OWN_ORDER)
    wait(tables)
    choose(1, halo_f, FAR_ORDER)
    wait(weights)
    for b in range(blocks):
        dense(cmat.at[1], cmat_t.at[1], b, cwt_f[b], ccols_f[b : b + 1, :], FAR_ORDER)

    second, third, fourth, fifth, sixth, sides, whole = {}, {}, {}, {}, {}, {}, {}
    n = len(cuts)

    def swap(c, sent, got, kept, sign, tag, value):
        span = pl.ds(*cuts[c])
        last = []
        for t in range(2):
            sent[0, t, span], kept[t, span] = value[t][:, :group], value[t][:, group : 2 * group]
            sent[1, t, span] = value[t][:, 2 * group : n_x]
            last.append(value[t][:, n_x:])
        sent[0, 2, span], sent[1, 2, span] = blend(last[0], last[1]), blend(last[1], last[0])
        return go(Pair(sent.at[:, :, span], got.at[:, :, span], sign, tag))

    def swapped(c, got, kept):
        span = pl.ds(*cuts[c])
        return [
            jnp.concatenate([
                got[0, 1 - t, span], kept[1 - t, span], got[1, 1 - t, span],
                blend(got[t, 2, span], got[1 - t, 2, span]),
            ], axis=1)
            for t in range(2)
        ]

    def adjoint(c):
        lo, count = cuts[c]
        span = pl.ds(lo, count)
        here = within(tx, lo, count)
        wait(crossed[c])
        z = [
            zp[mine(lo, count)] + scatter(0, [r1o[g, span] for g in (0, 2, 1)]),
            zf[span] + scatter(1, [near[g, tx, here] for g in (0, 2, 1)]),
        ]
        z = [stacked(item) for item in z]
        second[c] = swap(c, s2, r2, loc2, 1, "b", [apply(z[t], cmat.at[t], n_own, n_slot) for t in range(2)])
        for t in range(2):
            bown[t, span] = apply(z[t], cmat.at[t], 0, n_own)

    def middle(c):
        span = pl.ds(*cuts[c])
        wait(second[c])
        slots = swapped(c, r2, loc2)
        w = [stacked(bown[t, span] + scatter(t, [slots[t]])) for t in range(2)]
        third[c] = swap(c, s3, r3, loc3, -1, "w", [gather(t, w[t][1], 0, n_slot) for t in range(2)])
        for t in range(2):
            vacc[t, span] = apply_t(w[t], cmat_t.at[t], 0, n_own)

    def forward(c):
        lo, count = cuts[c]
        span, part = pl.ds(lo, count), pl.ds(lo // 2, count // 2)
        wait(third[c])
        slots = swapped(c, r3, loc3)
        v = [None, None]
        for t in (1, 0):
            v[t] = vacc[t, span] + apply_t(stacked(slots[t]), cmat_t.at[t], n_own, n_slot)
            vacc[t, span] = v[t]
            if t:
                whole[c] = go(Flow(vacc.at[1, span], v_r.at[span], ("z", c)))
        value = gather(0, stacked(v[0])[1], 0, n_slot)
        s4o[0, span], r4o[2, span], s4o[1, span] = (value[:, g * group : (g + 1) * group] for g in range(3))
        sides[c] = go(Pair(s4o.at[:, span], r4o.at[0:2, span], -1, "s"))
        s6[0, 2, part], s6[1, 2, part] = packed(value[:, n_x:])
        value = gather(1, stacked(v[1])[1], 0, n_x)
        loc6[span] = value[:, group : 2 * group]
        for q in range(2):
            rows_q = slice(q * (count // 2), (q + 1) * (count // 2))
            s6[0, q, part], s6[1, q, part] = value[rows_q, :group], value[rows_q, 2 * group :]

    def leave(c):
        span = pl.ds(*cuts[c])
        wait(sides[c])
        sixth[c] = go(Flow(r4o.at[:, span], r4x.at[:, span], ("g", c)))

    def joined(c, count):
        lo = cuts[c][0]
        end = sum(cuts[c + count - 1])
        return pl.ds(lo // 2, (end - lo) // 2)

    def spare(c, count):
        part = joined(c, count)
        fourth[c] = go(Pair(s6.at[:, :, part], r6.at[:, :, part], -1, "b" if c else "f"))

    def relay(c, count=1):
        for k in range(c, c + count):
            wait(whole[k])
            lo, width = cuts[k]
            part = pl.ds(lo // 2, width // 2)
            s5[0, part], s5[1, part] = packed(gather(0, stacked(v_r[pl.ds(lo, width)])[1], n_x, group))
        part = joined(c, count)
        fifth[c] = go(Pair(s5.at[:, part], r5.at[:, part], -1, ("t0", "t1", "x")[len(fifth)]))

    def finish(q, c, stages=(0, 1)):
        lo, count = cuts[c]
        span, part = pl.ds(lo, count), pl.ds(lo // 2, count // 2)
        place = theirs(lo, count) if q else mine(lo, count)
        if 0 in stages:
            wait(fifth.get(c, ()) if q else fourth.get(c, ()))
            last = unpacked(r5[0, part], r5[1, part]) if q else unpacked(r6[0, 2, part], r6[1, 2, part])
            main = v_r[span] if q else vacc[0, span]
        if 1 in stages and q:
            wait(sixth[c])
            outer = [r4x[g, span] for g in (0, 2, 1)]
        elif 1 in stages:
            outer = [jnp.concatenate([r6[k, 0, part], r6[k, 1, part]], axis=0) for k in range(2)]
            outer.insert(1, loc6[span])
        if len(stages) == 2:
            both = stacked(jnp.concatenate([main, *outer, last], axis=1))
            out_t[place] = apply_t(both, imat_t, 0, extent)
        elif 0 in stages:
            out_t[place] = apply_t(stacked(main), imat_t, 0, n_own) + apply_t(stacked(last), imat_t, n_own + n_x, group)
        else:
            both = stacked(jnp.concatenate(outer, axis=1))
            out_t[place] = out_t[place] + apply_t(both, imat_t, n_own, n_x)

    def ready(r):
        return max([c for c in range(n) if half + cuts[c][0] < (r + 1) * tile], default=-1)

    def store(c):
        for r in range(feat // tile):
            if ready(r) == c:
                block = far * r + tx * (feat // tile - 1 - r)
                span = pl.ds(pl.multiple_of(block * tile, tile), tile)
                live = lax.broadcasted_iota(jnp.int32, (rows, tile), 0) < limit
                out_ref[:, span] = jnp.where(live, out_t[span].T, 0.0)

    for step in range(n + 3):
        order = ((adjoint, 0), (middle, 1), (leave, 3), (forward, 2))
        if step > n:
            order = ((forward, 2), (leave, 3))
        for stage, lag in order:
            if 0 <= step - lag < n:
                stage(step - lag)
        if step == n:
            spare(0, n - 2)
        if step == n + 1:
            relay(0, n - 2)
            spare(n - 2, 2)
            for c in range(n - 2):
                finish(0, c)
    relay(n - 2)
    finish(0, n - 2)
    relay(n - 1)
    for c in range(n - 2):
        finish(1, c)
    finish(0, n - 1)
    for c in range(-1, n - 2):
        store(c)
    finish(1, n - 2)
    store(n - 2)
    settle(sixth[n - 1] + fifth[n - 1])
    finish(1, n - 1, (0,))
    finish(1, n - 1, (1,))
    store(n - 1)
    settle()


def split(total, parts):
    unit = total // 16
    sizes = [16 * (unit // parts + (1 if k < unit % parts else 0)) for k in range(parts)]
    starts = [sum(sizes[:k]) for k in range(parts)]
    return tuple(zip(starts, sizes))


def pair_call(n_ty, ctrl, interp_wt, interp_cols, conv_wt, conv_cols, halo_index, valid):
    rows, feat = ctrl.shape[2:]
    n_own = conv_wt.shape[2] * conv_wt.shape[3]
    n_slot = halo_index.shape[2] * halo_index.shape[3]
    extent, group, half = n_own + n_slot, n_slot // 4, feat // 2
    cuts = split(half, 4)
    pin = functools.partial(pltpu.with_memory_space_constraint, memory_space=pltpu.HBM)
    hbm = pl.BlockSpec(memory_space=pltpu.HBM)
    vmem = pl.BlockSpec(memory_space=pltpu.VMEM)

    def f32(*shape):
        return pltpu.VMEM(shape, F32)

    def bf16(*shape):
        return pltpu.VMEM(shape, BF16)

    scratch = [
        *[pltpu.VMEM(item.shape[2:], jnp.int32) for item in (interp_cols, conv_cols, halo_index)],
        f32(rows, feat), f32(*interp_wt.shape[2:]), f32(*conv_wt.shape[2:]), f32(*conv_wt.shape[2:]),
        pltpu.VMEM(conv_cols.shape[2:], jnp.int32), pltpu.VMEM(halo_index.shape[2:], jnp.int32),
        bf16(2, feat, rows), bf16(2, rows, extent), bf16(2, extent, rows),
        bf16(2, 2, n_own, extent), bf16(2, 2, extent, n_own), bf16(2, n_own, n_slot), bf16(2, n_slot, n_own),
        f32(feat, n_own), f32(2, 3, half, group), f32(3, 3, half, group),
        f32(half, n_own), f32(3, half, group), f32(2, half, n_own),
        f32(2, 3, half, group), f32(2, 3, half, group), f32(2, half, group),
        f32(2, 3, half, group), f32(2, 3, half, group), f32(2, half, group), f32(2, half, n_own),
        f32(2, half, group), f32(3, half, group), f32(3, half, group), f32(half, n_own),
        f32(2, 3, half // 2, group), f32(2, 3, half // 2, group), f32(half, group),
        f32(2, half // 2, group), f32(2, half // 2, group),
        f32(feat, rows),
    ]
    dma = pltpu.SemaphoreType.DMA
    scratch += [dma((7 + 2 * len(cuts),)), dma((5 + 8 * len(cuts),)), dma((6,))]
    return pl.pallas_call(
        functools.partial(pair_kernel, n_ty, cuts),
        out_shape=jax.ShapeDtypeStruct((rows, feat), F32),
        in_specs=[pl.BlockSpec(memory_space=pltpu.SMEM)] + [hbm] * 6,
        out_specs=vmem,
        scratch_shapes=scratch,
        compiler_params=pltpu.CompilerParams(
            collective_id=0, has_side_effects=True, vmem_limit_bytes=52 * 1024 * 1024
        ),
    )(
        valid, pin(ctrl[0, 0]), pin(interp_wt[0, 0]), pin(interp_cols[0, 0]), pin(conv_wt[0, 0]),
        pin(conv_cols[0, 0]), pin(halo_index[0, 0]),
    )


def pairs_fit(n_tx, ctrl, halo_index):
    slot = halo_index.shape[3]
    return n_tx == 2 and halo_index.shape[2] == 8 and slot == 64 and ctrl.shape[3] % 128 == 0


def solution(mesh):
    n_ty, n_tx = mesh.shape["ty"], mesh.shape["tx"]

    def body(ctrl, interp_wt, interp_cols, conv_wt, conv_cols, halo_index, valid):
        rows, feat = ctrl.shape[2:]
        n_own = conv_wt.shape[2] * conv_wt.shape[3]
        n_slot = halo_index.shape[2] * halo_index.shape[3]
        extent = n_own + n_slot
        if pairs_fit(n_tx, ctrl, halo_index) and rows == n_own:
            args = ctrl, interp_wt, interp_cols, conv_wt, conv_cols, halo_index, valid
            return pair_call(n_ty, *args)[None, None]
        tiles = feat // 128
        first = 128 * max(tiles - tiles // 2, 1)
        chunks = ((0, first), (first, feat - first)) if feat > first else ((0, feat),)
        widths = [width for _, width in chunks]
        pin = functools.partial(pltpu.with_memory_space_constraint, memory_space=pltpu.HBM)
        hbm = pl.BlockSpec(memory_space=pltpu.HBM)
        vmem = pl.BlockSpec(memory_space=pltpu.VMEM)
        scratch = [
            pltpu.VMEM(interp_wt.shape[2:], F32),
            pltpu.VMEM(conv_wt.shape[2:], F32),
            pltpu.VMEM((2, rows, extent), BF16),
            pltpu.VMEM((2, extent, rows), BF16),
            pltpu.VMEM((2, n_own, extent), BF16),
            pltpu.VMEM((2, extent, n_own), BF16),
            pltpu.VMEM((n_slot, n_own), BF16),
            pltpu.VMEM((n_own, n_slot), BF16),
        ]
        assert rows == n_own
        scratch += [pltpu.VMEM((n_own, width), F32) for width in widths]
        scratch += [pltpu.VMEM((2, extent, width), BF16) for width in widths]
        scratch += [pltpu.VMEM((n_slot, width), F32) for _ in range(8) for width in widths]
        scratch += [pltpu.SemaphoreType.DMA((4, len(chunks), 8))] * 2
        scratch += [pltpu.SemaphoreType.DMA((2 + len(chunks),)), pltpu.SemaphoreType.DMA((len(chunks),))]
        out = pl.pallas_call(
            functools.partial(kernel, n_ty, n_tx, chunks),
            out_shape=jax.ShapeDtypeStruct((rows, feat), F32),
            in_specs=[pl.BlockSpec(memory_space=pltpu.SMEM), hbm, hbm, vmem, hbm, vmem, vmem],
            out_specs=pl.BlockSpec(memory_space=pl.ANY),
            scratch_shapes=scratch,
            compiler_params=pltpu.CompilerParams(
                collective_id=0, has_side_effects=True, vmem_limit_bytes=44 * 1024 * 1024
            ),
        )(
            valid, pin(ctrl[0, 0]), pin(interp_wt[0, 0]), pin(interp_cols[0, 0]), pin(conv_wt[0, 0]),
            pin(conv_cols[0, 0]), pin(halo_index[0, 0]),
        )
        return out[None, None]

    placed = (
        P("ty", "tx", None, None),
        P("ty", "tx", None, None, None),
        P("ty", "tx", None, None),
        P("ty", "tx", None, None, None),
        P("ty", "tx", None, None),
        P("ty", "tx", None, None),
        P("ty", "tx"),
    )
    return jax.shard_map(
        body, mesh=mesh, in_specs=placed, out_specs=P("ty", "tx", None, None), check_vma=False
    )
```
